256 devices in a mesh: tm: 8 (over x, core), gx: 4 (over y), gy: 8 (over z).
Axes of the slice: x: 4, y: 4, z: 8, core: 2. Of those that a mesh axis runs over, the one named last changes fastest.
Arguments:
- trajectory: float32 [16, 3, 256, 1024], P('tm', None, 'gy', 'gx'), may hold values from -3 to 3
- initial: float32 [3, 256, 1024], P(None, 'gy', 'gx'), may hold values from -3 to 3
Outputs:
- updated: float32 [16, 3, 256, 1024], P('tm', None, 'gy', 'gx')
- residual: float32 [16, 3, 256, 1024], P('tm', None, 'gy', 'gx')
The draws below stay inside these ranges and needn't reach their ends.
All inputs are finite; a program needn't handle non-finite values.
Results may differ from the reference program's by a relative error of at most 0.00023.
Values sent between devices are 32-bit elements; how exact they have to be, the bound alone decides.
A program may use at most 64 MiB of HBM per device.

```python
import math
import jax
import jax.numpy as jnp
from jax import lax

CHEB = 6
NT = 16
NLAT = 256
NLON = 1024


def level_of(own_key, shape, pieces, low, largest):
    def one(position, blocks):
        heights = jax.random.uniform(jax.random.fold_in(jax.random.fold_in(own_key, 6), position), (blocks,), jnp.float32, low / len(pieces), largest / len(pieces))
        return jnp.repeat(jnp.exp(heights), shape[position] // blocks).reshape((-1,) + (1,) * (len(shape) - position - 1))

    loudness = one(*pieces[0])
    for cut in pieces[1:]:
        loudness = loudness * one(*cut)
    return loudness


def normal_values(rng, shape, width, reach, pieces=(), held_as=jnp.bfloat16):
    array = width * jax.random.normal(rng, shape, jnp.float32)
    if pieces:
        array = array * level_of(rng, shape, pieces, -0.22, 0.18)
    return jnp.clip(array, -reach, reach).astype(held_as)


def setup_inputs(seed: int = 0) -> dict:
    keys = jax.random.split(jax.random.key(seed), 3)
    return {
        "trajectory": normal_values(keys[0], (NT, 3, NLAT, NLON), 0.5, 3.0, ((0, 8), (2, 8), (3, 4)), jnp.float32),
        "initial": normal_values(keys[1], (3, NLAT, NLON), 0.5, 3.0, ((1, 8), (2, 4)), jnp.float32),
    }


courant_x = 1.5
courant_y = 1.5
coriolis_mean = 0.3
coriolis_slope = 0.4
circulant = 0.1
spectrum_edge = 5.0
highest = lax.Precision.HIGHEST


def along_lon(fields):
    return jnp.roll(fields, -1, -1) - jnp.roll(fields, 1, -1)


def along_lat(fields):
    return jnp.roll(fields, -1, -2) - jnp.roll(fields, 1, -2)


def coriolis(start, count, extent):
    latitude = (start + lax.iota(jnp.int32, count)).astype(jnp.float32)
    return (coriolis_mean + coriolis_slope * ((latitude + 0.5) / extent - 0.5))[:, None]


def wave(fields, rotation):
    height, eastward, northward = fields[..., 0, :, :], fields[..., 1, :, :], fields[..., 2, :, :]
    height_rate = courant_x * along_lon(eastward) + courant_y * along_lat(northward)
    east_rate = courant_x * along_lon(height) - rotation * northward
    north_rate = courant_y * along_lat(height) + rotation * eastward
    return jnp.stack([height_rate, east_rate, north_rate], axis=-3)


def advect(fields):
    height, eastward, northward = fields[..., 0, :, :], fields[..., 1, :, :], fields[..., 2, :, :]
    height_rate = courant_x * along_lon(height * eastward) + courant_y * along_lat(height * northward)
    east_rate = eastward * (courant_x * along_lon(eastward)) + northward * (courant_y * along_lat(eastward))
    north_rate = eastward * (courant_x * along_lon(northward)) + northward * (courant_y * along_lat(northward))
    return jnp.stack([height_rate, east_rate, north_rate], axis=-3)


def phase_table(rows, columns, total):
    products = (rows[:, None] * columns[None, :]) % total
    return (2.0 * math.pi / total) * products.astype(jnp.float32)


def time_weights(times, total, signed):
    return jnp.exp((signed * math.log(circulant) / total) * times.astype(jnp.float32))


def frequency_shift(frequency, total):
    factor = math.exp(math.log(circulant) / total)
    angle = (2.0 * math.pi / total) * frequency.astype(jnp.float32)
    return (1.0 - factor * jnp.cos(angle), factor * jnp.sin(angle))


def complex_times(first, second):
    return (first[0] * second[0] - first[1] * second[1], first[0] * second[1] + first[1] * second[0])


def complex_divide(first, second):
    denominator = second[0] * second[0] + second[1] * second[1]
    return ((first[0] * second[0] + first[1] * second[1]) / denominator,
            (first[1] * second[0] - first[0] * second[1]) / denominator)


def chebyshev(rhs, shift, operator):
    sigma = complex_divide(shift, (0.0, spectrum_edge))
    rho_old = complex_divide((1.0, 0.0), sigma)
    update = complex_divide(rhs, shift)
    solution = update
    for iteration in range(CHEB):
        turned = operator(solution)
        shifted = complex_times(shift, solution)
        misfit = (rhs[0] - (shifted[0] + turned[0]), rhs[1] - (shifted[1] + turned[1]))
        rho_new = complex_divide((1.0, 0.0), (2.0 * sigma[0] - rho_old[0], 2.0 * sigma[1] - rho_old[1]))
        carry_coef = complex_times(rho_new, rho_old)
        misfit_coef = complex_divide((2.0 * rho_new[0], 2.0 * rho_new[1]), (0.0, spectrum_edge))
        first_part = complex_times(carry_coef, update)
        second_part = complex_times(misfit_coef, misfit)
        update = (first_part[0] + second_part[0], first_part[1] + second_part[1])
        solution = (solution[0] + update[0], solution[1] + update[1])
        rho_old = rho_new
    return solution


def reference(trajectory, initial):
    total, fieldcount, nlat, nlon = trajectory.shape
    rotation = coriolis(0, nlat, nlat)
    previous = jnp.concatenate([initial[None], trajectory[:-1]], axis=0)
    residual = trajectory - previous + wave(trajectory, rotation) + advect(trajectory)
    times = lax.iota(jnp.int32, total)
    scaled = residual * time_weights(times, total, 1.0)[:, None, None, None]
    flat = scaled.reshape(total, -1)
    table = phase_table(times, times, total)
    cosines = jnp.cos(table)
    sines = jnp.sin(table)
    spec_re = jnp.dot(cosines, flat, precision=highest).reshape(trajectory.shape)
    spec_im = (-jnp.dot(sines, flat, precision=highest)).reshape(trajectory.shape)

    def wave_pair(couple):
        return (wave(couple[0], rotation), wave(couple[1], rotation))

    def solve_one(packed):
        rhs_re, rhs_im, frequency = packed
        shift = frequency_shift(frequency, total)
        return chebyshev((rhs_re, rhs_im), shift, wave_pair)

    sol_re, sol_im = lax.map(solve_one, (spec_re, spec_im, times))
    back = (jnp.dot(cosines, sol_re.reshape(total, -1), precision=highest)
            - jnp.dot(sines, sol_im.reshape(total, -1), precision=highest)) / total
    correction = back.reshape(trajectory.shape) * time_weights(times, total, -1.0)[:, None, None, None]
    return trajectory - correction, residual
```

```python
import math

import jax
import jax.numpy as jnp
import numpy as np
from jax import lax
from jax.experimental import pallas as pl
from jax.experimental.pallas import tpu as pltpu
from jax.sharding import PartitionSpec as P

MESH = pl.DeviceIdType.MESH
F32 = jnp.float32

CHEB = 6
STEPS = 16
courant = 1.5
coriolis_mean = 0.3
coriolis_slope = 0.4
circulant = 0.1
spectrum_edge = 5.0

HALO = 8
ROWS = 32
TALL = ROWS + 2 * HALO
WRAPS = 1.0 / circulant


def power_table():
    beta = circulant ** (1.0 / STEPS)
    solved = np.zeros((STEPS, CHEB + 1), complex)
    for k in range(STEPS):
        theta = 2.0 * np.pi * k / STEPS
        shift = 1.0 - beta * np.cos(theta) + 1j * beta * np.sin(theta)
        edge = 1j * spectrum_edge
        sigma = shift / edge
        rho_old = 1.0 / sigma
        one = np.zeros(CHEB + 2, complex)
        one[0] = 1.0
        update = one / shift
        total = update.copy()
        for _ in range(CHEB):
            misfit = one - (shift * total + np.roll(total, 1))
            rho_new = 1.0 / (2.0 * sigma - rho_old)
            update = rho_new * rho_old * update + 2.0 * rho_new / edge * misfit
            total = total + update
            rho_old = rho_new
        solved[k] = total[: CHEB + 1]
    turns = np.exp(2j * np.pi / STEPS * np.outer(np.arange(STEPS), np.arange(STEPS)))
    table = (turns @ solved).real / STEPS
    return table * spectrum_edge ** np.arange(CHEB + 1)


TABLE = power_table()


def weight(delta, p, q, m):
    difference = 2 * delta + p - q
    return float(circulant ** (-difference / STEPS) * TABLE[difference % STEPS, m])


def kernel(
    traj, init, upd_out, res_out,
    state, powers, prev, strip_l, strip_r, edge_l, edge_r, res_buf,
    cross, crossed, own, relay, near_a, near_b, out_buf,
    load_sem, halo_s, halo_r, cross_s, cross_r, ring_s, ring_r, store_sem,
):
    tm, gx, gy = lax.axis_index("tm"), lax.axis_index("gx"), lax.axis_index("gy")
    n_tm, n_gx, n_gy = lax.axis_size("tm"), lax.axis_size("gx"), lax.axis_size("gy")
    core = lax.rem(tm, 2)
    east, west = lax.rem(gx + 1, n_gx), lax.rem(gx + n_gx - 1, n_gx)
    north, south = lax.rem(gy + 1, n_gy), lax.rem(gy + n_gy - 1, n_gy)
    after, before = lax.rem(tm + 1, n_tm), lax.rem(tm + n_tm - 1, n_tm)
    chip_up, chip_down = lax.rem(tm + 2, n_tm), lax.rem(tm + n_tm - 2, n_tm)
    partner = tm + 1 - 2 * core
    last = tm == n_tm - 1

    loads = []
    for lane in range(2):
        columns = pl.ds(128 * lane, 128)
        loads.append(pltpu.make_async_copy(
            traj.at[:, :, :, columns], state.at[pl.ds(0, 2), :, lane, pl.ds(HALO, ROWS), :], load_sem.at[2 * lane]))
        loads.append(pltpu.make_async_copy(
            init.at[:, :, columns], state.at[2, :, lane, pl.ds(HALO, ROWS), :], load_sem.at[2 * lane + 1]))
    for load in loads:
        load.start()

    around = [(tm, west, gy), (tm, east, gy), (tm, gx, south), (tm, gx, north),
              (tm, west, south), (tm, west, north), (tm, east, south), (tm, east, north)]
    peers = around + [(partner, gx, gy), (chip_up, gx, gy), (chip_down, gx, gy),
                      (jnp.where(core == 1, after, before), gx, gy)]
    barrier = pltpu.get_barrier_semaphore()
    for peer in peers:
        pl.semaphore_signal(barrier, inc=1, device_id=peer, device_id_type=MESH)

    for load in loads:
        load.wait()

    lane_id = lax.broadcasted_iota(jnp.int32, (TALL, 128), 1)
    packed_l = jnp.zeros((ROWS, 128), F32)
    packed_r = jnp.zeros((ROWS, 128), F32)
    for s in range(3):
        for f in range(3):
            spot = 8 * (3 * s + f)
            here = (lane_id[:ROWS] >= spot) & (lane_id[:ROWS] < spot + 8)
            left = state[s, f, 0, pl.ds(HALO, ROWS), :]
            right = state[s, f, 1, pl.ds(HALO, ROWS), :]
            packed_l = jnp.where(here, pltpu.roll(left, spot, 1) if spot else left, packed_l)
            packed_r = jnp.where(here, pltpu.roll(right, spot + 8, 1), packed_r)
    strip_l[...] = packed_l
    strip_r[...] = packed_r

    pl.semaphore_wait(barrier, len(peers))

    def remote(src, dst, send, recv, peer):
        return pltpu.make_async_remote_copy(
            src_ref=src, dst_ref=dst, send_sem=send, recv_sem=recv, device_id=peer, device_id_type=MESH)

    top, bottom, low, high = pl.ds(0, HALO), pl.ds(ROWS - HALO, HALO), pl.ds(HALO, HALO), pl.ds(ROWS, HALO)
    under, over = pl.ds(0, HALO), pl.ds(HALO + ROWS, HALO)
    both, cols = pl.ds(0, 2), pl.ds(0, 2)
    halo = [
        remote(strip_l.at[top], edge_r.at[over], halo_s.at[0], halo_r.at[0], (tm, west, south)),
        remote(strip_l.at[bottom], edge_r.at[under], halo_s.at[1], halo_r.at[1], (tm, west, north)),
        remote(strip_r.at[top], edge_l.at[over], halo_s.at[2], halo_r.at[2], (tm, east, south)),
        remote(strip_r.at[bottom], edge_l.at[under], halo_s.at[3], halo_r.at[3], (tm, east, north)),
        remote(strip_l, edge_r.at[pl.ds(HALO, ROWS)], halo_s.at[4], halo_r.at[4], (tm, west, gy)),
        remote(strip_r, edge_l.at[pl.ds(HALO, ROWS)], halo_s.at[5], halo_r.at[5], (tm, east, gy)),
        remote(state.at[both, :, cols, low, :], state.at[both, :, cols, over, :], halo_s.at[6], halo_r.at[6],
               (tm, gx, south)),
        remote(state.at[both, :, cols, high, :], state.at[both, :, cols, under, :], halo_s.at[7], halo_r.at[7],
               (tm, gx, north)),
    ]
    opening = [
        remote(state.at[2, :, cols, low, :], state.at[2, :, cols, over, :], halo_s.at[8], halo_r.at[8], (tm, gx, south)),
        remote(state.at[2, :, cols, high, :], state.at[2, :, cols, under, :], halo_s.at[9], halo_r.at[9],
               (tm, gx, north)),
    ]
    passed = remote(state.at[1, :, cols, pl.ds(HALO, ROWS), :], prev, halo_s.at[10], halo_r.at[10], (after, gx, gy))
    for copy in halo:
        copy.start()

    @pl.when(last)
    def _():
        for copy in opening:
            copy.start()

    passed.start()

    for copy in halo:
        copy.wait_recv()

    @pl.when(last)
    def _():
        for copy in opening:
            copy.wait_recv()

    for s in range(3):
        for f in range(3):
            spot = 8 * (3 * s + f)
            right = pltpu.roll(edge_r[...], (128 - spot) % 128, 1) if spot else edge_r[...]
            left = pltpu.roll(edge_l[...], 120 - spot, 1)
            state[s, f, 2, :, :] = jnp.where(lane_id < 64, right, left)

    row = (gy * ROWS - HALO + n_gy * ROWS + lax.broadcasted_iota(jnp.int32, (TALL, 128), 0)) % (n_gy * ROWS)
    rotation = coriolis_mean + coriolis_slope * ((row.astype(F32) + 0.5) / (n_gy * ROWS) - 0.5)

    first_lane, final_lane = lane_id == 0, lane_id == 127

    def dx(tiles):
        ahead = [pltpu.roll(t, 127, 1) for t in tiles]
        behind = [pltpu.roll(t, 1, 1) for t in tiles]
        return [jnp.where(final_lane, ahead[(l + 1) % 3], ahead[l]) - jnp.where(first_lane, behind[(l + 2) % 3], behind[l])
                for l in range(3)]

    def dy(tile):
        return pltpu.roll(tile, TALL - 1, 0) - pltpu.roll(tile, 1, 0)

    def start_fields(s, carry):
        h = [state[s, 0, l, :, :] for l in range(3)]
        u = [state[s, 1, l, :, :] for l in range(3)]
        v = [state[s, 2, l, :, :] for l in range(3)]
        flux = dx([u[l] + h[l] * u[l] for l in range(3)])
        slope_h, slope_u, slope_v = dx(h), dx(u), dx(v)
        for l in range(3):
            powers[0, s, 0, l, :, :] = h[l] + courant * (flux[l] + dy(v[l] + h[l] * v[l]))
            powers[0, s, 1, l, :, :] = u[l] + (
                courant * slope_h[l] - rotation * v[l] + courant * (u[l] * slope_u[l] + v[l] * dy(u[l])))
            powers[0, s, 2, l, :, :] = v[l] + (
                courant * dy(h[l]) + rotation * u[l] + courant * (u[l] * slope_v[l] + v[l] * dy(v[l])))
        return carry

    lax.fori_loop(0, 2, start_fields, 0)

    slot = jnp.where(last, 2, 1)
    factor = jnp.where(last, -WRAPS, -1.0).astype(F32)
    for f in range(3):
        for l in range(3):
            powers[0, 2, f, l, :, :] = factor * state[slot, f, l, :, :]
            powers[0, 1, f, l, :, :] = powers[0, 1, f, l, :, :] - state[0, f, l, :, :]

    step = courant / spectrum_edge
    turning = rotation * (1.0 / spectrum_edge)

    def next_power(m, carry):
        for q in range(3):
            h = [powers[m, q, 0, l, :, :] for l in range(3)]
            u = [powers[m, q, 1, l, :, :] for l in range(3)]
            v = [powers[m, q, 2, l, :, :] for l in range(3)]
            slope_h, slope_u = dx(h), dx(u)
            for l in range(3):
                powers[m + 1, q, 0, l, :, :] = step * (slope_u[l] + dy(v[l]))
                powers[m + 1, q, 1, l, :, :] = step * slope_h[l] - turning * v[l]
                powers[m + 1, q, 2, l, :, :] = step * dy(h[l]) + turning * u[l]
        return carry

    lax.fori_loop(0, CHEB, next_power, 0)

    PIECE = 16
    pieces = ROWS // PIECE

    def mix(f, wanted):
        def body(i, carry):
            l, t = i // pieces, i % pieces
            source = pl.ds(pl.multiple_of(HALO + PIECE * t, 8), PIECE)
            rows = pl.ds(pl.multiple_of(PIECE * t, 8), PIECE)
            terms = [[powers[m, q, f, l, source, :] for m in range(CHEB + 1)] for q in range(3)]
            for delta, p, store in wanted:
                total = None
                for q in range(3):
                    for m in range(CHEB + 1):
                        term = weight(delta, p, q, m) * terms[q][m]
                        total = term if total is None else total + term
                if delta:
                    total = total * jnp.where(tm + delta >= n_tm, circulant, 1.0).astype(F32)
                store(l, rows, total)
            return carry
        lax.fori_loop(0, 2 * pieces, body, 0)

    def into(ref, *index):
        def store(l, rows, value):
            ref[(*index, l, rows, slice(None))] = value
        return store

    def cross_copy(odd, f):
        where = lax.rem(odd + core, 4)
        return remote(cross.at[odd, f], crossed.at[where, f], cross_s.at[odd, f], cross_r.at[where, f],
                      (partner, gx, gy))

    def crossed_in(place, f):
        return remote(cross.at[place, f], crossed.at[place, f], cross_s.at[place, f], cross_r.at[place, f],
                      (partner, gx, gy))

    up, down = (chip_up, gx, gy), (chip_down, gx, gy)

    def ring_copy(stage, side, src, dst, f):
        return remote(src, dst, ring_s.at[stage, side, f], ring_r.at[stage, side, f], down if side else up)

    def far_copy(side, f):
        return ring_copy(0, side, own.at[0, f, side], relay.at[side, f], f)

    def near_copy(side, f):
        return ring_copy(1, side, own.at[1 + side, f, 1 - side], near_a.at[side, f], f)

    def relayed_copy(side, f):
        return ring_copy(2, side, own.at[1 + side, f, side], near_b.at[side, f], f)

    def m1(f, carry):
        mix(f, [(3, 0, into(cross, 1, f, 0)), (3, 1, into(cross, 1, f, 1)),
                (5, 0, into(cross, 2, f, 0)), (5, 1, into(cross, 2, f, 1))])
        cross_copy(1, f).start()
        cross_copy(2, f).start()
        return carry

    def m2(f, carry):
        mix(f, [(4, 0, into(own, 0, f, 0)), (4, 1, into(own, 0, f, 1))])
        return carry

    def s1(f, carry):
        crossed_in(2, f).wait_recv()
        own[0, f] = own[0, f] + crossed[2, f]
        far_copy(0, f).start()
        far_copy(1, f).start()
        return carry

    def m3(f, carry):
        mix(f, [(1, 0, into(cross, 0, f, 0)), (1, 1, into(cross, 0, f, 1)),
                (7, 0, into(cross, 3, f, 0)), (7, 1, into(cross, 3, f, 1))])
        cross_copy(0, f).start()
        cross_copy(3, f).start()
        return carry

    def m4(f, carry):
        mix(f, [(2, 0, into(own, 1, f, 0)), (2, 1, into(own, 1, f, 1)),
                (6, 0, into(own, 2, f, 0)), (6, 1, into(own, 2, f, 1))])
        return carry

    def s2(f, carry):
        crossed_in(1, f).wait_recv()
        crossed_in(3, f).wait_recv()
        own[1, f] = own[1, f] + crossed[1, f]
        own[2, f] = own[2, f] + crossed[3, f]
        near_copy(0, f).start()
        near_copy(1, f).start()
        return carry

    def s3(f, carry):
        for side in range(2):
            far_copy(side, f).wait_recv()
            own[1 + side, f, side] = own[1 + side, f, side] + relay[side, f]
            relayed_copy(side, f).start()
        return carry

    def m5(f, carry):
        mix(f, [(0, 0, into(own, 3, f, 0)), (0, 1, into(own, 3, f, 1))])
        crossed_in(0, f).wait_recv()
        for p in range(2):
            for l in range(2):
                out_buf[p, f, l] = state[p, f, l, pl.ds(HALO, ROWS), :] - (own[3, f, p, l] + crossed[0, f, p, l])
        return carry

    lax.fori_loop(0, 3, m1, 0)
    lax.fori_loop(0, 3, m2, 0)
    lax.fori_loop(0, 3, s1, 0)
    lax.fori_loop(0, 3, m3, 0)
    lax.fori_loop(0, 3, m4, 0)
    lax.fori_loop(0, 3, s2, 0)
    lax.fori_loop(0, 3, s3, 0)
    lax.fori_loop(0, 3, m5, 0)

    passed.wait_recv()
    for f in range(3):
        for l in range(2):
            before_first = jnp.where(tm == 0, state[2, f, l, pl.ds(HALO, ROWS), :], prev[f, l])
            res_buf[0, f, l] = powers[0, 0, f, l, pl.ds(HALO, ROWS), :] - before_first
            res_buf[1, f, l] = powers[0, 1, f, l, pl.ds(HALO, ROWS), :]
    stores = [pltpu.make_async_copy(res_buf.at[:, :, l], res_out.at[:, :, :, pl.ds(128 * l, 128)], store_sem.at[l])
              for l in range(2)]
    for store in stores:
        store.start()

    def finish(f, carry):
        for side in range(2):
            near_copy(side, f).wait_recv()
            relayed_copy(side, f).wait_recv()
        for l in range(2):
            out_buf[0, f, l] = out_buf[0, f, l] - (near_b[0, f, l] + near_a[1, f, l])
            out_buf[1, f, l] = out_buf[1, f, l] - (near_a[0, f, l] + near_b[1, f, l])
        return carry

    lax.fori_loop(0, 3, finish, 0)
    ends = [pltpu.make_async_copy(out_buf.at[:, :, l], upd_out.at[:, :, :, pl.ds(128 * l, 128)], store_sem.at[2 + l])
            for l in range(2)]
    for end in ends:
        end.start()

    for copy in halo:
        copy.wait_send()

    @pl.when(last)
    def _():
        for copy in opening:
            copy.wait_send()

    passed.wait_send()

    def drain(f, carry):
        for odd in range(4):
            cross_copy(odd, f).wait_send()
        for side in range(2):
            far_copy(side, f).wait_send()
            near_copy(side, f).wait_send()
            relayed_copy(side, f).wait_send()
        return carry

    lax.fori_loop(0, 3, drain, 0)
    for store in stores + ends:
        store.wait()


def shards(trajectory, initial):
    whole = jax.ShapeDtypeStruct(trajectory.shape, F32)
    anywhere = pl.BlockSpec(memory_space=pl.ANY)
    dma = pltpu.SemaphoreType.DMA
    return pl.pallas_call(
        kernel,
        out_shape=(whole, whole),
        in_specs=[anywhere, anywhere],
        out_specs=(anywhere, anywhere),
        scratch_shapes=[
            pltpu.VMEM((3, 3, 3, TALL, 128), F32),
            pltpu.VMEM((CHEB + 1, 3, 3, 3, TALL, 128), F32),
            pltpu.VMEM((3, 2, ROWS, 128), F32),
            pltpu.VMEM((ROWS, 128), F32),
            pltpu.VMEM((ROWS, 128), F32),
            pltpu.VMEM((TALL, 128), F32),
            pltpu.VMEM((TALL, 128), F32),
            pltpu.VMEM((2, 3, 2, ROWS, 128), F32),
            pltpu.VMEM((4, 3, 2, 2, ROWS, 128), F32),
            pltpu.VMEM((4, 3, 2, 2, ROWS, 128), F32),
            pltpu.VMEM((4, 3, 2, 2, ROWS, 128), F32),
            pltpu.VMEM((2, 3, 2, ROWS, 128), F32),
            pltpu.VMEM((2, 3, 2, ROWS, 128), F32),
            pltpu.VMEM((2, 3, 2, ROWS, 128), F32),
            pltpu.VMEM((2, 3, 2, ROWS, 128), F32),
            dma((4,)),
            dma((11,)),
            dma((11,)),
            dma((4, 3)),
            dma((4, 3)),
            dma((3, 2, 3)),
            dma((3, 2, 3)),
            dma((4,)),
        ],
        compiler_params=pltpu.CompilerParams(collective_id=0, has_side_effects=True),
        name="paradiag",
    )(trajectory, initial)


def solution(mesh):
    in_specs = (P("tm", None, "gy", "gx"), P(None, "gy", "gx"))
    out_specs = (P("tm", None, "gy", "gx"), P("tm", None, "gy", "gx"))
    return jax.shard_map(shards, mesh=mesh, in_specs=in_specs, out_specs=out_specs, check_vma=False)
```

```python
import math

import jax
import jax.numpy as jnp
import numpy as np
from jax import lax
from jax.experimental import pallas as pl
from jax.experimental.pallas import tpu as pltpu
from jax.sharding import PartitionSpec as P

MESH = pl.DeviceIdType.MESH
F32 = jnp.float32

CHEB = 6
STEPS = 16
courant = 1.5
coriolis_mean = 0.3
coriolis_slope = 0.4
circulant = 0.1
spectrum_edge = 5.0

HALO = 8
ROWS = 32
TALL = ROWS + 2 * HALO
EDGE = 8
BASE = EDGE + HALO
DEEP = TALL + 2 * EDGE
WRAPS = 1.0 / circulant
OPPOSITE = (1, 0, 3, 2, 5, 4, 7, 6, 8, 10, 9, 11)


def power_table():
    beta = circulant ** (1.0 / STEPS)
    solved = np.zeros((STEPS, CHEB + 1), complex)
    for k in range(STEPS):
        theta = 2.0 * np.pi * k / STEPS
        shift = 1.0 - beta * np.cos(theta) + 1j * beta * np.sin(theta)
        edge = 1j * spectrum_edge
        sigma = shift / edge
        rho_old = 1.0 / sigma
        one = np.zeros(CHEB + 2, complex)
        one[0] = 1.0
        update = one / shift
        total = update.copy()
        for _ in range(CHEB):
            misfit = one - (shift * total + np.roll(total, 1))
            rho_new = 1.0 / (2.0 * sigma - rho_old)
            update = rho_new * rho_old * update + 2.0 * rho_new / edge * misfit
            total = total + update
            rho_old = rho_new
        solved[k] = total[: CHEB + 1]
    turns = np.exp(2j * np.pi / STEPS * np.outer(np.arange(STEPS), np.arange(STEPS)))
    table = (turns @ solved).real / STEPS
    return table * courant ** np.arange(CHEB + 1)


TABLE = power_table()


def weight(delta, p, q, m):
    difference = 2 * delta + p - q
    return float(circulant ** (-difference / STEPS) * TABLE[difference % STEPS, m])


def kernel(
    traj, init, out_buf, res_buf,
    state, powers, rotation, prev, strip_l, strip_r, edge_l, edge_r,
    cross, crossed, own, relay, near_a, near_b,
    ready, load_sem, halo_s, halo_r, cross_s, cross_r, ring_s, ring_r,
):
    tm, gx, gy = lax.axis_index("tm"), lax.axis_index("gx"), lax.axis_index("gy")
    n_tm, n_gx, n_gy = lax.axis_size("tm"), lax.axis_size("gx"), lax.axis_size("gy")
    core = lax.rem(tm, 2)
    east, west = lax.rem(gx + 1, n_gx), lax.rem(gx + n_gx - 1, n_gx)
    north, south = lax.rem(gy + 1, n_gy), lax.rem(gy + n_gy - 1, n_gy)
    after, before = lax.rem(tm + 1, n_tm), lax.rem(tm + n_tm - 1, n_tm)
    chip_up, chip_down = lax.rem(tm + 2, n_tm), lax.rem(tm + n_tm - 2, n_tm)
    partner = tm + 1 - 2 * core
    last = tm == n_tm - 1

    loads = []
    for lane in range(2):
        columns = pl.ds(128 * lane, 128)
        loads.append(pltpu.make_async_copy(
            traj.at[:, :, :, columns], state.at[pl.ds(0, 2), :, lane, pl.ds(BASE, ROWS), :], load_sem.at[2 * lane]))
        loads.append(pltpu.make_async_copy(
            init.at[:, :, columns], state.at[2, :, lane, pl.ds(BASE, ROWS), :], load_sem.at[2 * lane + 1]))
    for load in loads:
        load.start()

    def arrival(t, x, y):
        chip, seat = t // 2, t % 2
        by_x = chip + (chip + 3) // 4
        by_y = x + x // 2 - 2 * (x // 3)
        by_z = jnp.minimum(2 * y, 66 - 9 * y)
        return ((by_x + by_y + by_z) * 2 + 1 - seat) * 256 + t * 32 + x * 8 + y

    across = jnp.where(core == 1, after, before)
    peers = [(tm, east, gy), (tm, west, gy), (tm, gx, north), (tm, gx, south),
             (tm, east, north), (tm, west, south), (tm, east, south), (tm, west, north),
             (partner, gx, gy), (chip_up, gx, gy), (chip_down, gx, gy), (across, gx, gy)]
    mine = arrival(tm, gx, gy)
    earlier = [(arrival(*peer) < mine).astype(jnp.int32) for peer in peers]

    barrier = pltpu.get_barrier_semaphore()
    for peer, sooner in zip(peers, earlier, strict=True):
        @pl.when(sooner == 0)
        def _(peer=peer):
            pl.semaphore_signal(barrier, inc=1, device_id=peer, device_id_type=MESH)

    sooner_count = sum(earlier)

    @pl.when(sooner_count > 0)
    def _():
        pl.semaphore_wait(barrier, sooner_count)

    for i, (peer, sooner) in enumerate(zip(peers, earlier, strict=True)):
        @pl.when(sooner == 1)
        def _(i=i, peer=peer):
            pl.semaphore_signal(ready.at[OPPOSITE[i]], inc=1, device_id=peer, device_id_type=MESH)

    def met(i):
        @pl.when(earlier[i] == 0)
        def _():
            pl.semaphore_wait(ready.at[i], 1)

    for load in loads:
        load.wait()

    lane_id = lax.broadcasted_iota(jnp.int32, (TALL, 128), 1)
    packed_l = jnp.zeros((ROWS, 128), F32)
    packed_r = jnp.zeros((ROWS, 128), F32)
    for s in range(3):
        for f in range(3):
            spot = 8 * (3 * s + f)
            here = (lane_id[:ROWS] >= spot) & (lane_id[:ROWS] < spot + 8)
            left = state[s, f, 0, pl.ds(BASE, ROWS), :]
            right = state[s, f, 1, pl.ds(BASE, ROWS), :]
            packed_l = jnp.where(here, pltpu.roll(left, spot, 1) if spot else left, packed_l)
            packed_r = jnp.where(here, pltpu.roll(right, spot + 8, 1), packed_r)
    strip_l[...] = packed_l
    strip_r[...] = packed_r

    def remote(src, dst, send, recv, peer):
        return pltpu.make_async_remote_copy(
            src_ref=src, dst_ref=dst, send_sem=send, recv_sem=recv, device_id=peer, device_id_type=MESH)

    top, bottom, low, high = pl.ds(0, HALO), pl.ds(ROWS - HALO, HALO), pl.ds(BASE, HALO), pl.ds(EDGE + ROWS, HALO)
    first, final = pl.ds(0, HALO), pl.ds(HALO + ROWS, HALO)
    under, over = pl.ds(EDGE, HALO), pl.ds(BASE + ROWS, HALO)
    both, cols = pl.ds(0, 2), pl.ds(0, 2)
    def halo_copy(i, src, dst):
        return remote(src, dst, halo_s.at[i], halo_r.at[OPPOSITE[i]], peers[i])

    def halo_in(i, src, dst):
        return remote(src, dst, halo_s.at[i], halo_r.at[i], peers[i])

    middle = pl.ds(HALO, ROWS)
    sides = [
        (strip_r, edge_l.at[middle], strip_l, edge_r.at[middle]),
        (strip_l, edge_r.at[middle], strip_r, edge_l.at[middle]),
        (state.at[both, :, cols, high, :], state.at[both, :, cols, under, :],
         state.at[both, :, cols, low, :], state.at[both, :, cols, over, :]),
        (state.at[both, :, cols, low, :], state.at[both, :, cols, over, :],
         state.at[both, :, cols, high, :], state.at[both, :, cols, under, :]),
        (strip_r.at[bottom], edge_l.at[first], strip_l.at[top], edge_r.at[final]),
        (strip_l.at[top], edge_r.at[final], strip_r.at[bottom], edge_l.at[first]),
        (strip_r.at[top], edge_l.at[final], strip_l.at[bottom], edge_r.at[first]),
        (strip_l.at[bottom], edge_r.at[first], strip_r.at[top], edge_l.at[final]),
    ]
    halo = [halo_copy(i, sides[i][0], sides[i][1]) for i in range(8)]
    arriving = [halo_in(i, sides[i][2], sides[i][3]) for i in range(8)]
    opening = [
        remote(state.at[2, :, cols, high, :], state.at[2, :, cols, under, :], halo_s.at[8], halo_r.at[8],
               (tm, gx, north)),
        remote(state.at[2, :, cols, low, :], state.at[2, :, cols, over, :], halo_s.at[9], halo_r.at[9], (tm, gx, south)),
    ]
    passed = remote(state.at[1, :, cols, pl.ds(BASE, ROWS), :], prev, halo_s.at[10], halo_r.at[10], (after, gx, gy))
    for i in range(8):
        @pl.when(earlier[i] == 1)
        def _(i=i):
            halo[i].start()
    for i in range(8):
        @pl.when(earlier[i] == 0)
        def _(i=i):
            pl.semaphore_wait(ready.at[i], 1)
            halo[i].start()

    @pl.when(last)
    def _():
        for copy in opening:
            copy.start()

    for i in range(8, 12):
        met(i)
    passed.start()

    for copy in arriving:
        copy.wait_recv()

    @pl.when(last)
    def _():
        for copy in opening:
            copy.wait_recv()

    tall = pl.ds(EDGE, TALL)
    for s in range(3):
        for f in range(3):
            spot = 8 * (3 * s + f)
            right = pltpu.roll(edge_r[...], (128 - spot) % 128, 1) if spot else edge_r[...]
            left = pltpu.roll(edge_l[...], 120 - spot, 1)
            state[s, f, 2, tall, :] = jnp.where(lane_id < 64, right, left)

    row = (gy * ROWS - HALO + n_gy * ROWS + lax.broadcasted_iota(jnp.int32, (TALL, 128), 0)) % (n_gy * ROWS)
    latitude = coriolis_mean + coriolis_slope * ((row.astype(F32) + 0.5) / (n_gy * ROWS) - 0.5)
    rotation[...] = latitude * (1.0 / courant)

    first_lane, final_lane = lane_id == 0, lane_id == 127

    def dx(tiles):
        ahead = [pltpu.roll(t, 127, 1) for t in tiles]
        behind = [pltpu.roll(t, 1, 1) for t in tiles]
        return [jnp.where(final_lane, ahead[(l + 1) % 3], ahead[l]) - jnp.where(first_lane, behind[(l + 2) % 3], behind[l])
                for l in range(3)]

    above, below = pl.ds(EDGE + 1, TALL), pl.ds(EDGE - 1, TALL)

    def start_fields(s, carry):
        h = [state[s, 0, l, tall, :] for l in range(3)]
        u = [state[s, 1, l, tall, :] for l in range(3)]
        v = [state[s, 2, l, tall, :] for l in range(3)]
        turn = rotation[...]
        flux = dx([u[l] + h[l] * u[l] for l in range(3)])
        slope_h, slope_u, slope_v = dx(h), dx(u), dx(v)
        for l in range(3):
            (ha, hb), (ua, ub), (va, vb) = [(state[s, f, l, above, :], state[s, f, l, below, :]) for f in range(3)]
            powers[0, s, 0, l, tall, :] = h[l] + courant * (flux[l] + ((va + ha * va) - (vb + hb * vb)))
            powers[0, s, 1, l, tall, :] = u[l] + courant * (
                slope_h[l] - turn * v[l] + (u[l] * slope_u[l] + v[l] * (ua - ub)))
            powers[0, s, 2, l, tall, :] = v[l] + courant * (
                (ha - hb) + turn * u[l] + (u[l] * slope_v[l] + v[l] * (va - vb)))
        return carry

    lax.fori_loop(0, 2, start_fields, 0)

    slot = jnp.where(last, 2, 1)
    factor = jnp.where(last, -WRAPS, -1.0).astype(F32)
    for f in range(3):
        for l in range(3):
            powers[0, 2, f, l, tall, :] = factor * state[slot, f, l, tall, :]
            powers[0, 1, f, l, tall, :] = powers[0, 1, f, l, tall, :] - state[0, f, l, tall, :]

    def next_power(m, carry):
        for q in range(3):
            h = [powers[m, q, 0, l, tall, :] for l in range(3)]
            u = [powers[m, q, 1, l, tall, :] for l in range(3)]
            slope_h, slope_u = dx(h), dx(u)
            turn = rotation[...]
            for l in range(3):
                ha, hb = powers[m, q, 0, l, above, :], powers[m, q, 0, l, below, :]
                va, vb = powers[m, q, 2, l, above, :], powers[m, q, 2, l, below, :]
                v = powers[m, q, 2, l, tall, :]
                powers[m + 1, q, 0, l, tall, :] = slope_u[l] + (va - vb)
                powers[m + 1, q, 1, l, tall, :] = slope_h[l] - turn * v
                powers[m + 1, q, 2, l, tall, :] = (ha - hb) + turn * u[l]
        return carry

    lax.fori_loop(0, CHEB, next_power, 0)

    PIECE = 16
    pieces = ROWS // PIECE

    def mix(f, wanted):
        def body(i, carry):
            l, t = i // pieces, i % pieces
            source = pl.ds(pl.multiple_of(BASE + PIECE * t, 8), PIECE)
            rows = pl.ds(pl.multiple_of(PIECE * t, 8), PIECE)
            terms = [[powers[m, q, f, l, source, :] for m in range(CHEB + 1)] for q in range(3)]
            for delta, p, store in wanted:
                total = None
                for q in range(3):
                    for m in range(CHEB + 1):
                        term = weight(delta, p, q, m) * terms[q][m]
                        total = term if total is None else total + term
                if delta:
                    total = total * jnp.where(tm + delta >= n_tm, circulant, 1.0).astype(F32)
                store(l, rows, total)
            return carry
        lax.fori_loop(0, 2 * pieces, body, 0)

    def into(ref, *index):
        def store(l, rows, value):
            ref[(*index, l, rows, slice(None))] = value
        return store

    def cross_copy(odd, f):
        where = lax.rem(odd + core, 4)
        return remote(cross.at[odd, f], crossed.at[where, f], cross_s.at[odd, f], cross_r.at[where, f],
                      (partner, gx, gy))

    def crossed_in(place, f):
        return remote(cross.at[place, f], crossed.at[place, f], cross_s.at[place, f], cross_r.at[place, f],
                      (partner, gx, gy))

    up, down = (chip_up, gx, gy), (chip_down, gx, gy)

    def ring_copy(stage, side, src, dst, f):
        return remote(src, dst, ring_s.at[stage, side, f], ring_r.at[stage, side, f], down if side else up)

    def far_copy(side, f):
        return ring_copy(0, side, own.at[0, f, side], relay.at[side, f], f)

    def near_copy(side, f):
        return ring_copy(1, side, own.at[1 + side, f, 1 - side], near_a.at[side, f], f)

    def relayed_copy(side, f):
        return ring_copy(2, side, own.at[1 + side, f, side], near_b.at[side, f], f)

    def m1(f, carry):
        mix(f, [(3, 0, into(cross, 1, f, 0)), (3, 1, into(cross, 1, f, 1)),
                (5, 0, into(cross, 2, f, 0)), (5, 1, into(cross, 2, f, 1))])
        cross_copy(1, f).start()
        cross_copy(2, f).start()
        return carry

    def m2(f, carry):
        mix(f, [(4, 0, into(own, 0, f, 0)), (4, 1, into(own, 0, f, 1))])
        return carry

    def s1(f, carry):
        crossed_in(2, f).wait_recv()
        own[0, f] = own[0, f] + crossed[2, f]
        far_copy(0, f).start()
        far_copy(1, f).start()
        return carry

    def m3(f, carry):
        mix(f, [(1, 0, into(cross, 0, f, 0)), (1, 1, into(cross, 0, f, 1)),
                (7, 0, into(cross, 3, f, 0)), (7, 1, into(cross, 3, f, 1))])
        cross_copy(0, f).start()
        cross_copy(3, f).start()
        return carry

    def m4(f, carry):
        mix(f, [(2, 0, into(own, 1, f, 0)), (2, 1, into(own, 1, f, 1)),
                (6, 0, into(own, 2, f, 0)), (6, 1, into(own, 2, f, 1))])
        return carry

    def s2(f, carry):
        crossed_in(1, f).wait_recv()
        crossed_in(3, f).wait_recv()
        own[1, f] = own[1, f] + crossed[1, f]
        own[2, f] = own[2, f] + crossed[3, f]
        near_copy(0, f).start()
        near_copy(1, f).start()
        return carry

    def s3(f, carry):
        for side in range(2):
            far_copy(side, f).wait_recv()
            own[1 + side, f, side] = own[1 + side, f, side] + relay[side, f]
            relayed_copy(side, f).start()
        return carry

    def m5(f, carry):
        mix(f, [(0, 0, into(own, 3, f, 0)), (0, 1, into(own, 3, f, 1))])
        crossed_in(0, f).wait_recv()
        for p in range(2):
            for l in range(2):
                out_buf[p, f, l] = state[p, f, l, pl.ds(BASE, ROWS), :] - (own[3, f, p, l] + crossed[0, f, p, l])
        return carry

    lax.fori_loop(0, 3, m1, 0)
    lax.fori_loop(0, 3, m2, 0)
    lax.fori_loop(0, 3, s1, 0)
    lax.fori_loop(0, 3, m3, 0)
    lax.fori_loop(0, 3, m4, 0)
    lax.fori_loop(0, 3, s2, 0)
    lax.fori_loop(0, 3, s3, 0)
    lax.fori_loop(0, 3, m5, 0)

    passed.wait_recv()
    for f in range(3):
        for l in range(2):
            before_first = jnp.where(tm == 0, state[2, f, l, pl.ds(BASE, ROWS), :], prev[f, l])
            res_buf[0, f, l] = powers[0, 0, f, l, pl.ds(BASE, ROWS), :] - before_first
            res_buf[1, f, l] = powers[0, 1, f, l, pl.ds(BASE, ROWS), :]
    def finish(f, carry):
        for side in range(2):
            near_copy(side, f).wait_recv()
            relayed_copy(side, f).wait_recv()
        for l in range(2):
            out_buf[0, f, l] = out_buf[0, f, l] - (near_b[0, f, l] + near_a[1, f, l])
            out_buf[1, f, l] = out_buf[1, f, l] - (near_a[0, f, l] + near_b[1, f, l])
        return carry

    lax.fori_loop(0, 3, finish, 0)
    for copy in halo:
        copy.wait_send()

    @pl.when(last)
    def _():
        for copy in opening:
            copy.wait_send()

    passed.wait_send()

    def drain(f, carry):
        for odd in range(4):
            cross_copy(odd, f).wait_send()
        for side in range(2):
            far_copy(side, f).wait_send()
            near_copy(side, f).wait_send()
            relayed_copy(side, f).wait_send()
        return carry

    lax.fori_loop(0, 3, drain, 0)


def put_out(upd_in, res_in, upd_out, res_out, sem):
    copies = []
    for l in range(2):
        columns = pl.ds(128 * l, 128)
        copies.append(pltpu.make_async_copy(upd_in.at[:, :, l], upd_out.at[:, :, :, columns], sem.at[l]))
        copies.append(pltpu.make_async_copy(res_in.at[:, :, l], res_out.at[:, :, :, columns], sem.at[2 + l]))
    for copy in copies:
        copy.start()
    for copy in copies:
        copy.wait()


def shards(trajectory, initial):
    whole = jax.ShapeDtypeStruct(trajectory.shape, F32)
    anywhere = pl.BlockSpec(memory_space=pl.ANY)
    slow = pl.BlockSpec(memory_space=pltpu.HBM)
    fast = pl.BlockSpec(memory_space=pltpu.VMEM)
    dma = pltpu.SemaphoreType.DMA
    tiles = pltpu.VMEM((2, 3, 2, ROWS, 128), F32)
    updated, residual = pl.pallas_call(
        kernel,
        out_shape=(tiles, tiles),
        in_specs=[slow, slow],
        out_specs=(fast, fast),
        scratch_shapes=[
            pltpu.VMEM((3, 3, 3, DEEP, 128), F32),
            pltpu.VMEM((CHEB + 1, 3, 3, 3, DEEP, 128), F32),
            pltpu.VMEM((TALL, 128), F32),
            pltpu.VMEM((3, 2, ROWS, 128), F32),
            pltpu.VMEM((ROWS, 128), F32),
            pltpu.VMEM((ROWS, 128), F32),
            pltpu.VMEM((TALL, 128), F32),
            pltpu.VMEM((TALL, 128), F32),
            pltpu.VMEM((4, 3, 2, 2, ROWS, 128), F32),
            pltpu.VMEM((4, 3, 2, 2, ROWS, 128), F32),
            pltpu.VMEM((4, 3, 2, 2, ROWS, 128), F32),
            pltpu.VMEM((2, 3, 2, ROWS, 128), F32),
            pltpu.VMEM((2, 3, 2, ROWS, 128), F32),
            pltpu.VMEM((2, 3, 2, ROWS, 128), F32),
            pltpu.SemaphoreType.REGULAR((12,)),
            dma((4,)),
            dma((11,)),
            dma((11,)),
            dma((4, 3)),
            dma((4, 3)),
            dma((3, 2, 3)),
            dma((3, 2, 3)),
        ],
        compiler_params=pltpu.CompilerParams(collective_id=0, has_side_effects=True),
        name="paradiag",
    )(trajectory, initial)
    return pl.pallas_call(
        put_out,
        out_shape=(whole, whole),
        in_specs=[anywhere, anywhere],
        out_specs=(anywhere, anywhere),
        scratch_shapes=[dma((4,))],
        compiler_params=pltpu.CompilerParams(vmem_limit_bytes=4 << 20),
        name="put_out",
    )(updated, residual)


def solution(mesh):
    in_specs = (P("tm", None, "gy", "gx"), P(None, "gy", "gx"))
    out_specs = (P("tm", None, "gy", "gx"), P("tm", None, "gy", "gx"))
    return jax.shard_map(shards, mesh=mesh, in_specs=in_specs, out_specs=out_specs, check_vma=False)
```

```python
import math

import jax
import jax.numpy as jnp
import numpy as np
from jax import lax
from jax.experimental import pallas as pl
from jax.experimental.pallas import tpu as pltpu
from jax.sharding import PartitionSpec as P

MESH = pl.DeviceIdType.MESH
F32 = jnp.float32

CHEB = 6
STEPS = 16
courant = 1.5
coriolis_mean = 0.3
coriolis_slope = 0.4
circulant = 0.1
spectrum_edge = 5.0

HALO = 8
ROWS = 32
TALL = ROWS + 2 * HALO
EDGE = 8
BASE = EDGE + HALO
DEEP = TALL + 2 * EDGE
WRAPS = 1.0 / circulant
OPPOSITE = (1, 0, 5, 6, 7, 2, 3, 4, 8, 8, 8, 8)
(LOAD, HALO_S, HALO_R, OPEN_S, OPEN_R, PASS_S, PASS_R, CROSS_S, RING_S, CROSS_FAR, CROSS_NEAR, CROSS_OWN, RING_FAR,
 RING_END, N_SEM) = (0, 1, 2, 3, 4, 5, 6, 7, 8, 9, 12, 15, 16, 19, 22)


def power_table():
    beta = circulant ** (1.0 / STEPS)
    solved = np.zeros((STEPS, CHEB + 1), complex)
    for k in range(STEPS):
        theta = 2.0 * np.pi * k / STEPS
        shift = 1.0 - beta * np.cos(theta) + 1j * beta * np.sin(theta)
        edge = 1j * spectrum_edge
        sigma = shift / edge
        rho_old = 1.0 / sigma
        one = np.zeros(CHEB + 2, complex)
        one[0] = 1.0
        update = one / shift
        total = update.copy()
        for _ in range(CHEB):
            misfit = one - (shift * total + np.roll(total, 1))
            rho_new = 1.0 / (2.0 * sigma - rho_old)
            update = rho_new * rho_old * update + 2.0 * rho_new / edge * misfit
            total = total + update
            rho_old = rho_new
        solved[k] = total[: CHEB + 1]
    turns = np.exp(2j * np.pi / STEPS * np.outer(np.arange(STEPS), np.arange(STEPS)))
    table = (turns @ solved).real / STEPS
    return table * courant ** np.arange(CHEB + 1)


TABLE = power_table()


def weight(delta, p, q, m):
    difference = 2 * delta + p - q
    return float(circulant ** (-difference / STEPS) * TABLE[difference % STEPS, m])


def kernel(
    traj, init, out_buf, res_buf,
    state, powers, rotation, prev, strip_l, strip_r, edge_l, edge_r,
    cross, crossed, own, relay, near_a, near_b,
    ready, sem,
):
    tm, gx, gy = lax.axis_index("tm"), lax.axis_index("gx"), lax.axis_index("gy")
    n_tm, n_gx, n_gy = lax.axis_size("tm"), lax.axis_size("gx"), lax.axis_size("gy")
    core = lax.rem(tm, 2)
    east, west = lax.rem(gx + 1, n_gx), lax.rem(gx + n_gx - 1, n_gx)
    north, south = lax.rem(gy + 1, n_gy), lax.rem(gy + n_gy - 1, n_gy)
    after, before = lax.rem(tm + 1, n_tm), lax.rem(tm + n_tm - 1, n_tm)
    chip_up, chip_down = lax.rem(tm + 2, n_tm), lax.rem(tm + n_tm - 2, n_tm)
    partner = tm + 1 - 2 * core
    last = tm == n_tm - 1

    loads = []
    for lane in range(2):
        columns = pl.ds(128 * lane, 128)
        loads.append(pltpu.make_async_copy(
            traj.at[:, :, :, columns], state.at[pl.ds(0, 2), :, lane, pl.ds(BASE, ROWS), :], sem.at[LOAD]))
        loads.append(pltpu.make_async_copy(
            init.at[:, :, columns], state.at[2, :, lane, pl.ds(BASE, ROWS), :], sem.at[LOAD]))
    for load in loads:
        load.start()
    loaded = state.at[:, :, pl.ds(0, 2), pl.ds(BASE, ROWS), :]

    def arrival(t, x, y):
        by_z = jnp.minimum(2 * y + 2 * jnp.minimum(y, 1), 11)
        return (t // 2 + x + by_z + 1 - t % 2) * 256 + t * 32 + x * 8 + y

    across = jnp.where(core == 1, after, before)
    peers = [(tm, east, gy), (tm, west, gy), (tm, gx, north), (tm, east, north), (tm, west, north),
             (tm, gx, south), (tm, west, south), (tm, east, south),
             (partner, gx, gy), (chip_up, gx, gy), (chip_down, gx, gy), (across, gx, gy)]
    mine = arrival(tm, gx, gy)
    earlier = [(arrival(*peer) < mine).astype(jnp.int32) for peer in peers]

    barrier = pltpu.get_barrier_semaphore()
    for peer, sooner in zip(peers, earlier, strict=True):
        @pl.when(sooner == 0)
        def _(peer=peer):
            pl.semaphore_signal(barrier, inc=1, device_id=peer, device_id_type=MESH)

    sooner_count = sum(earlier)

    @pl.when(sooner_count > 0)
    def _():
        pl.semaphore_wait(barrier, sooner_count)

    for i, (peer, sooner) in enumerate(zip(peers, earlier, strict=True)):
        @pl.when(sooner == 1)
        def _(i=i, peer=peer):
            pl.semaphore_signal(ready.at[OPPOSITE[i]], inc=1, device_id=peer, device_id_type=MESH)

    pltpu.make_async_copy(loaded, loaded, sem.at[LOAD]).wait()

    lane_id = lax.broadcasted_iota(jnp.int32, (TALL, 128), 1)
    packed_l = jnp.zeros((ROWS, 128), F32)
    packed_r = jnp.zeros((ROWS, 128), F32)
    for s in range(3):
        for f in range(3):
            spot = 8 * (3 * s + f)
            here = (lane_id[:ROWS] >= spot) & (lane_id[:ROWS] < spot + 8)
            left = state[s, f, 0, pl.ds(BASE, ROWS), :]
            right = state[s, f, 1, pl.ds(BASE, ROWS), :]
            packed_l = jnp.where(here, pltpu.roll(left, spot, 1) if spot else left, packed_l)
            packed_r = jnp.where(here, pltpu.roll(right, spot + 8, 1), packed_r)
    strip_l[...] = packed_l
    strip_r[...] = packed_r

    def remote(src, dst, send, recv, peer):
        return pltpu.make_async_remote_copy(
            src_ref=src, dst_ref=dst, send_sem=send, recv_sem=recv, device_id=peer, device_id_type=MESH)

    top, bottom, low, high = pl.ds(0, HALO), pl.ds(ROWS - HALO, HALO), pl.ds(BASE, HALO), pl.ds(EDGE + ROWS, HALO)
    first, final = pl.ds(0, HALO), pl.ds(HALO + ROWS, HALO)
    under, over = pl.ds(EDGE, HALO), pl.ds(BASE + ROWS, HALO)
    both, cols = pl.ds(0, 2), pl.ds(0, 2)
    middle = pl.ds(HALO, ROWS)
    sides = [
        (strip_r, edge_l.at[middle]),
        (strip_l, edge_r.at[middle]),
        (state.at[both, :, cols, high, :], state.at[both, :, cols, under, :]),
        (strip_r.at[bottom], edge_l.at[first]),
        (strip_l.at[bottom], edge_r.at[first]),
        (state.at[both, :, cols, low, :], state.at[both, :, cols, over, :]),
        (strip_l.at[top], edge_r.at[final]),
        (strip_r.at[top], edge_l.at[final]),
    ]
    halo = [remote(src, dst, sem.at[HALO_S], sem.at[HALO_R], peers[i]) for i, (src, dst) in enumerate(sides)]
    opening = [
        remote(state.at[2, :, cols, high, :], state.at[2, :, cols, under, :], sem.at[OPEN_S], sem.at[OPEN_R],
               (tm, gx, north)),
        remote(state.at[2, :, cols, low, :], state.at[2, :, cols, over, :], sem.at[OPEN_S], sem.at[OPEN_R],
               (tm, gx, south)),
    ]
    passed = remote(state.at[1, :, cols, pl.ds(BASE, ROWS), :], prev, sem.at[PASS_S], sem.at[PASS_R], (after, gx, gy))
    for i in range(8):
        @pl.when(earlier[i] == 1)
        def _(i=i):
            halo[i].start()
    for i in range(8):
        @pl.when(earlier[i] == 0)
        def _(i=i):
            pl.semaphore_wait(ready.at[i], 1)
            halo[i].start()

    @pl.when(last)
    def _():
        for copy in opening:
            copy.start()

    later_count = 4 - sum(earlier[8:])

    @pl.when(later_count > 0)
    def _():
        pl.semaphore_wait(ready.at[8], later_count)

    passed.start()

    def await_bytes(ref, i):
        pltpu.make_async_copy(ref, ref, sem.at[i]).wait()

    halo_bytes, opening_bytes = state.at[:, :, 0, pl.ds(0, ROWS), :], state.at[2, :, cols, pl.ds(0, 2 * HALO), :]
    await_bytes(halo_bytes, HALO_R)

    @pl.when(last)
    def _():
        await_bytes(opening_bytes, OPEN_R)

    tall = pl.ds(EDGE, TALL)
    for s in range(3):
        for f in range(3):
            spot = 8 * (3 * s + f)
            right = pltpu.roll(edge_r[...], (128 - spot) % 128, 1) if spot else edge_r[...]
            left = pltpu.roll(edge_l[...], 120 - spot, 1)
            state[s, f, 2, tall, :] = jnp.where(lane_id < 64, right, left)

    row = (gy * ROWS - HALO + n_gy * ROWS + lax.broadcasted_iota(jnp.int32, (TALL, 128), 0)) % (n_gy * ROWS)
    latitude = coriolis_mean + coriolis_slope * ((row.astype(F32) + 0.5) / (n_gy * ROWS) - 0.5)
    rotation[...] = latitude * (1.0 / courant)


    def dx(tiles):
        ahead = [pltpu.roll(t, 127, 1) for t in tiles]
        behind = [pltpu.roll(t, 1, 1) for t in tiles]
        lane = lane_id[: tiles[0].shape[0]]
        return [jnp.where(lane == 127, ahead[(l + 1) % 3], ahead[l]) - jnp.where(lane == 0, behind[(l + 2) % 3], behind[l])
                for l in range(3)]

    above, below = pl.ds(EDGE + 1, TALL), pl.ds(EDGE - 1, TALL)

    def start_fields(s, carry):
        h = [state[s, 0, l, tall, :] for l in range(3)]
        u = [state[s, 1, l, tall, :] for l in range(3)]
        v = [state[s, 2, l, tall, :] for l in range(3)]
        turn = rotation[...]
        flux = dx([u[l] + h[l] * u[l] for l in range(3)])
        slope_h, slope_u, slope_v = dx(h), dx(u), dx(v)
        for l in range(3):
            (ha, hb), (ua, ub), (va, vb) = [(state[s, f, l, above, :], state[s, f, l, below, :]) for f in range(3)]
            powers[0, s, 0, l, tall, :] = h[l] + courant * (flux[l] + ((va + ha * va) - (vb + hb * vb)))
            powers[0, s, 1, l, tall, :] = u[l] + courant * (
                slope_h[l] - turn * v[l] + (u[l] * slope_u[l] + v[l] * (ua - ub)))
            powers[0, s, 2, l, tall, :] = v[l] + courant * (
                (ha - hb) + turn * u[l] + (u[l] * slope_v[l] + v[l] * (va - vb)))
        return carry

    lax.fori_loop(0, 2, start_fields, 0)

    slot = jnp.where(last, 2, 1)
    factor = jnp.where(last, -WRAPS, -1.0).astype(F32)
    for f in range(3):
        for l in range(3):
            powers[0, 2, f, l, tall, :] = factor * state[slot, f, l, tall, :]
            powers[0, 1, f, l, tall, :] = powers[0, 1, f, l, tall, :] - state[0, f, l, tall, :]

    def next_power(m, carry):
        for q in range(3):
            h = [powers[m, q, 0, l, tall, :] for l in range(3)]
            u = [powers[m, q, 1, l, tall, :] for l in range(3)]
            slope_h, slope_u = dx(h), dx(u)
            turn = rotation[...]
            for l in range(3):
                ha, hb = powers[m, q, 0, l, above, :], powers[m, q, 0, l, below, :]
                va, vb = powers[m, q, 2, l, above, :], powers[m, q, 2, l, below, :]
                v = powers[m, q, 2, l, tall, :]
                powers[m + 1, q, 0, l, tall, :] = slope_u[l] + (va - vb)
                powers[m + 1, q, 1, l, tall, :] = slope_h[l] - turn * v
                powers[m + 1, q, 2, l, tall, :] = (ha - hb) + turn * u[l]
        return carry

    lax.fori_loop(0, CHEB - 1, next_power, 0)

    block, block_up, block_down = pl.ds(BASE, ROWS), pl.ds(BASE + 1, ROWS), pl.ds(BASE - 1, ROWS)
    m = CHEB - 1
    for q in range(3):
        h = [powers[m, q, 0, l, block, :] for l in range(3)]
        u = [powers[m, q, 1, l, block, :] for l in range(3)]
        slope_h, slope_u = dx(h), dx(u)
        turn = rotation[pl.ds(HALO, ROWS), :]
        for l in range(2):
            ha, hb = powers[m, q, 0, l, block_up, :], powers[m, q, 0, l, block_down, :]
            va, vb = powers[m, q, 2, l, block_up, :], powers[m, q, 2, l, block_down, :]
            v = powers[m, q, 2, l, block, :]
            powers[m + 1, q, 0, l, block, :] = slope_u[l] + (va - vb)
            powers[m + 1, q, 1, l, block, :] = slope_h[l] - turn * v
            powers[m + 1, q, 2, l, block, :] = (ha - hb) + turn * u[l]

    def mix(f, wanted):
        def body(l, carry):
            totals = [None] * len(wanted)
            for q in range(3):
                for m in range(CHEB + 1):
                    value = powers[m, q, f, l, block, :]
                    for i, (delta, p, _, _) in enumerate(wanted):
                        term = weight(delta, p, q, m) * value
                        totals[i] = term if totals[i] is None else totals[i] + term
            for (delta, p, ref, index), total in zip(wanted, totals, strict=True):
                if delta:
                    total = total * jnp.where(tm + delta >= n_tm, circulant, 1.0).astype(F32)
                ref[(*index, l)] = total
            return carry
        lax.fori_loop(0, 2, body, 0)

    def both_steps(delta, ref, *index):
        return [(delta, p, ref, (*index, p)) for p in range(2)]

    def send_across(place, f):
        i = {0: CROSS_OWN, 1: CROSS_NEAR + f, 2: CROSS_FAR + f, 3: CROSS_NEAR + f}[place]
        remote(cross.at[place, f], crossed.at[place, f], sem.at[CROSS_S], sem.at[i], (partner, gx, gy)).start()

    def odd_delta(seat, place):
        return (2 * place + 1 - 2 * seat) % 8

    def for_partner(f, places):
        for seat in range(2):
            @pl.when(core == seat)
            def _(seat=seat):
                mix(f, [w for place in places for w in both_steps(odd_delta(seat, place), cross, place, f)])
        for place in places:
            send_across(place, f)

    up, down = (chip_up, gx, gy), (chip_down, gx, gy)

    def send_ring(i, side, src, dst):
        remote(src, dst, sem.at[RING_S], sem.at[i], down if side else up).start()

    def far_odd(f, carry):
        for_partner(f, (2,))
        return carry

    def far_even(f, carry):
        mix(f, both_steps(4, own, 0, f))
        return carry

    def far_out(f, carry):
        for_partner(f, (1, 3))
        await_bytes(crossed.at[2, f], CROSS_FAR + f)
        own[0, f] = own[0, f] + crossed[2, f]
        for side in range(2):
            send_ring(RING_FAR + f, side, own.at[0, f, side], relay.at[side, f])
        return carry

    def near_out(f, carry):
        mix(f, both_steps(2, own, 1, f) + both_steps(6, own, 2, f))
        await_bytes(crossed.at[pl.ds(0, 2), f], CROSS_NEAR + f)
        own[1, f] = own[1, f] + crossed[1, f]
        own[2, f] = own[2, f] + crossed[3, f]
        for side in range(2):
            send_ring(RING_END + f, side, own.at[1 + side, f, 1 - side], near_a.at[side, f])
        return carry

    def here_odd(f, carry):
        for_partner(f, (0,))
        return carry

    def here_even(f, carry):
        mix(f, both_steps(0, own, 3, f))
        return carry

    def relay_out(f, carry):
        await_bytes(relay.at[:, f], RING_FAR + f)
        for side in range(2):
            own[1 + side, f, side] = own[1 + side, f, side] + relay[side, f]
            send_ring(RING_END + f, side, own.at[1 + side, f, side], near_b.at[side, f])
        return carry

    lax.fori_loop(0, 3, far_odd, 0)
    lax.fori_loop(0, 3, far_even, 0)
    lax.fori_loop(0, 3, far_out, 0)
    lax.fori_loop(0, 3, near_out, 0)
    lax.fori_loop(0, 3, here_odd, 0)
    lax.fori_loop(0, 3, here_even, 0)
    lax.fori_loop(0, 3, relay_out, 0)

    await_bytes(prev, PASS_R)
    await_bytes(crossed.at[0], CROSS_OWN)
    for f in range(3):
        for l in range(2):
            before_first = jnp.where(tm == 0, state[2, f, l, block, :], prev[f, l])
            res_buf[0, f, l] = powers[0, 0, f, l, block, :] - before_first
            res_buf[1, f, l] = powers[0, 1, f, l, block, :]
            for p in range(2):
                out_buf[p, f, l] = state[p, f, l, block, :] - (own[3, f, p, l] + crossed[0, f, p, l])

    await_bytes(halo_bytes, HALO_S)

    @pl.when(last)
    def _():
        await_bytes(opening_bytes, OPEN_S)

    await_bytes(prev, PASS_S)
    await_bytes(cross, CROSS_S)

    def finish(f, carry):
        await_bytes(own.at[pl.ds(0, 2), f], RING_END + f)
        for l in range(2):
            out_buf[0, f, l] = out_buf[0, f, l] - (near_b[0, f, l] + near_a[1, f, l])
            out_buf[1, f, l] = out_buf[1, f, l] - (near_a[0, f, l] + near_b[1, f, l])
        return carry

    lax.fori_loop(0, 3, finish, 0)
    await_bytes(own.at[pl.ds(0, 3)], RING_S)


def put_out(upd_in, res_in, upd_out, res_out, sem):
    copies = []
    for l in range(2):
        columns = pl.ds(128 * l, 128)
        copies.append(pltpu.make_async_copy(upd_in.at[:, :, l], upd_out.at[:, :, :, columns], sem.at[l]))
        copies.append(pltpu.make_async_copy(res_in.at[:, :, l], res_out.at[:, :, :, columns], sem.at[2 + l]))
    for copy in copies:
        copy.start()
    for copy in copies:
        copy.wait()


def shards(trajectory, initial):
    whole = jax.ShapeDtypeStruct(trajectory.shape, F32)
    anywhere = pl.BlockSpec(memory_space=pl.ANY)
    slow = pl.BlockSpec(memory_space=pltpu.HBM)
    fast = pl.BlockSpec(memory_space=pltpu.VMEM)
    dma = pltpu.SemaphoreType.DMA
    tiles = pltpu.VMEM((2, 3, 2, ROWS, 128), F32)
    updated, residual = pl.pallas_call(
        kernel,
        out_shape=(tiles, tiles),
        in_specs=[slow, slow],
        out_specs=(fast, fast),
        scratch_shapes=[
            pltpu.VMEM((3, 3, 3, DEEP, 128), F32),
            pltpu.VMEM((CHEB + 1, 3, 3, 3, DEEP, 128), F32),
            pltpu.VMEM((TALL, 128), F32),
            pltpu.VMEM((3, 2, ROWS, 128), F32),
            pltpu.VMEM((ROWS, 128), F32),
            pltpu.VMEM((ROWS, 128), F32),
            pltpu.VMEM((TALL, 128), F32),
            pltpu.VMEM((TALL, 128), F32),
            pltpu.VMEM((4, 3, 2, 2, ROWS, 128), F32),
            pltpu.VMEM((4, 3, 2, 2, ROWS, 128), F32),
            pltpu.VMEM((4, 3, 2, 2, ROWS, 128), F32),
            pltpu.VMEM((2, 3, 2, ROWS, 128), F32),
            pltpu.VMEM((2, 3, 2, ROWS, 128), F32),
            pltpu.VMEM((2, 3, 2, ROWS, 128), F32),
            pltpu.SemaphoreType.REGULAR((9,)),
            dma((N_SEM,)),
        ],
        compiler_params=pltpu.CompilerParams(collective_id=0, has_side_effects=True),
        name="paradiag",
    )(trajectory, initial)
    return pl.pallas_call(
        put_out,
        out_shape=(whole, whole),
        in_specs=[anywhere, anywhere],
        out_specs=(anywhere, anywhere),
        scratch_shapes=[dma((4,))],
        compiler_params=pltpu.CompilerParams(vmem_limit_bytes=4 << 20),
        name="put_out",
    )(updated, residual)


def solution(mesh):
    in_specs = (P("tm", None, "gy", "gx"), P(None, "gy", "gx"))
    out_specs = (P("tm", None, "gy", "gx"), P("tm", None, "gy", "gx"))
    return jax.shard_map(shards, mesh=mesh, in_specs=in_specs, out_specs=out_specs, check_vma=False)
```

```python
import math

import jax
import jax.numpy as jnp
import numpy as np
from jax import lax
from jax.experimental import pallas as pl
from jax.experimental.pallas import tpu as pltpu
from jax.sharding import PartitionSpec as P

MESH = pl.DeviceIdType.MESH
F32 = jnp.float32

CHEB = 6
STEPS = 16
courant = 1.5
coriolis_mean = 0.3
coriolis_slope = 0.4
circulant = 0.1
spectrum_edge = 5.0

HALO = 8
ROWS = 32
TALL = ROWS + 2 * HALO
EDGE = 8
BASE = EDGE + HALO
DEEP = TALL + 2 * EDGE
WRAPS = 1.0 / circulant
OPPOSITE = (1, 0, 5, 6, 7, 2, 3, 4, 8, 8, 8, 8)
MOST, REST = 24, 8
(LOAD, HALO_S, HALO_Y, HALO_SIDE, OPEN_S, OPEN_SIDE, PASS_S, PASS_R, CROSS_S, RING_S, CROSS_FAR, CROSS_NEAR, CROSS_OWN, RING_FAR,
 RING_END, N_SEM) = (0, 1, 2, 3, 5, 6, 8, 9, 10, 11, 12, 16, 20, 21, 25, 29)


def power_table():
    beta = circulant ** (1.0 / STEPS)
    solved = np.zeros((STEPS, CHEB + 1), complex)
    for k in range(STEPS):
        theta = 2.0 * np.pi * k / STEPS
        shift = 1.0 - beta * np.cos(theta) + 1j * beta * np.sin(theta)
        edge = 1j * spectrum_edge
        sigma = shift / edge
        rho_old = 1.0 / sigma
        one = np.zeros(CHEB + 2, complex)
        one[0] = 1.0
        update = one / shift
        total = update.copy()
        for _ in range(CHEB):
            misfit = one - (shift * total + np.roll(total, 1))
            rho_new = 1.0 / (2.0 * sigma - rho_old)
            update = rho_new * rho_old * update + 2.0 * rho_new / edge * misfit
            total = total + update
            rho_old = rho_new
        solved[k] = total[: CHEB + 1]
    turns = np.exp(2j * np.pi / STEPS * np.outer(np.arange(STEPS), np.arange(STEPS)))
    table = (turns @ solved).real / STEPS
    return table * courant ** np.arange(CHEB + 1)


TABLE = power_table()


def weight(delta, p, q, m):
    difference = 2 * delta + p - q
    return float(circulant ** (-difference / STEPS) * TABLE[difference % STEPS, m])


def kernel(
    traj, init, out_buf, res_buf,
    state, powers, rotation, prev, strip_l, strip_r, edge_l, edge_r,
    side_in, cross, crossed, own, relay, near_a, near_b,
    ready, sem,
):
    tm, gx, gy = lax.axis_index("tm"), lax.axis_index("gx"), lax.axis_index("gy")
    n_tm, n_gx, n_gy = lax.axis_size("tm"), lax.axis_size("gx"), lax.axis_size("gy")
    core = lax.rem(tm, 2)
    east, west = lax.rem(gx + 1, n_gx), lax.rem(gx + n_gx - 1, n_gx)
    north, south = lax.rem(gy + 1, n_gy), lax.rem(gy + n_gy - 1, n_gy)
    after, before = lax.rem(tm + 1, n_tm), lax.rem(tm + n_tm - 1, n_tm)
    chip_up, chip_down = lax.rem(tm + 2, n_tm), lax.rem(tm + n_tm - 2, n_tm)
    partner = tm + 1 - 2 * core
    last = tm == n_tm - 1

    loads = []
    for lane in range(2):
        columns = pl.ds(128 * lane, 128)
        loads.append(pltpu.make_async_copy(
            traj.at[:, :, :, columns], state.at[pl.ds(0, 2), :, lane, pl.ds(BASE, ROWS), :], sem.at[LOAD]))
        loads.append(pltpu.make_async_copy(
            init.at[:, :, columns], state.at[2, :, lane, pl.ds(BASE, ROWS), :], sem.at[LOAD]))
    for load in loads:
        load.start()
    loaded = state.at[:, :, pl.ds(0, 2), pl.ds(BASE, ROWS), :]

    def arrival(t, x, y):
        by_z = jnp.minimum(2 * y + 2 * jnp.minimum(y, 1), 11)
        return (t // 2 + x + by_z + 1 - t % 2) * 256 + t * 32 + x * 8 + y

    across = jnp.where(core == 1, after, before)
    peers = [(tm, east, gy), (tm, west, gy), (tm, gx, north), (tm, east, north), (tm, west, north),
             (tm, gx, south), (tm, west, south), (tm, east, south),
             (partner, gx, gy), (chip_up, gx, gy), (chip_down, gx, gy), (across, gx, gy)]
    mine = arrival(tm, gx, gy)
    earlier = [(arrival(*peer) < mine).astype(jnp.int32) for peer in peers]

    barrier = pltpu.get_barrier_semaphore()
    for peer, sooner in zip(peers, earlier, strict=True):
        @pl.when(sooner == 0)
        def _(peer=peer):
            pl.semaphore_signal(barrier, inc=1, device_id=peer, device_id_type=MESH)

    sooner_count = sum(earlier)

    @pl.when(sooner_count > 0)
    def _():
        pl.semaphore_wait(barrier, sooner_count)

    for i, (peer, sooner) in enumerate(zip(peers, earlier, strict=True)):
        @pl.when(sooner == 1)
        def _(i=i, peer=peer):
            pl.semaphore_signal(ready.at[OPPOSITE[i]], inc=1, device_id=peer, device_id_type=MESH)

    pltpu.make_async_copy(loaded, loaded, sem.at[LOAD]).wait()

    lane_id = lax.broadcasted_iota(jnp.int32, (TALL, 128), 1)
    packed_l = jnp.zeros((ROWS, 128), F32)
    packed_r = jnp.zeros((ROWS, 128), F32)
    for s in range(3):
        for f in range(3):
            spot = 8 * (3 * s + f)
            here = (lane_id[:ROWS] >= spot) & (lane_id[:ROWS] < spot + 8)
            left = state[s, f, 0, pl.ds(BASE, ROWS), :]
            right = state[s, f, 1, pl.ds(BASE, ROWS), :]
            packed_l = jnp.where(here, pltpu.roll(left, spot, 1) if spot else left, packed_l)
            packed_r = jnp.where(here, pltpu.roll(right, spot + 8, 1), packed_r)
    strip_l[...] = packed_l
    strip_r[...] = packed_r

    def remote(src, dst, send, recv, peer):
        return pltpu.make_async_remote_copy(
            src_ref=src, dst_ref=dst, send_sem=send, recv_sem=recv, device_id=peer, device_id_type=MESH)

    top, bottom, low, high = pl.ds(0, HALO), pl.ds(ROWS - HALO, HALO), pl.ds(BASE, HALO), pl.ds(EDGE + ROWS, HALO)
    first, final = pl.ds(0, HALO), pl.ds(HALO + ROWS, HALO)
    both, cols = pl.ds(0, 2), pl.ds(0, 2)
    middle = pl.ds(HALO, ROWS)
    sides = [
        (strip_r, edge_l.at[middle]),
        (strip_l, edge_r.at[middle]),
        (state.at[both, :, cols, high, :], side_in.at[0, both]),
        (strip_r.at[bottom], edge_l.at[first]),
        (strip_l.at[bottom], edge_r.at[first]),
        (state.at[both, :, cols, low, :], side_in.at[1, both]),
        (strip_l.at[top], edge_r.at[final]),
        (strip_r.at[top], edge_l.at[final]),
    ]
    seats = (HALO_Y, HALO_Y, HALO_SIDE, HALO_SIDE, HALO_SIDE, HALO_SIDE + 1, HALO_SIDE + 1, HALO_SIDE + 1)
    halo = [remote(src, dst, sem.at[HALO_S], sem.at[seats[i]], peers[i]) for i, (src, dst) in enumerate(sides)]
    opening = [
        remote(state.at[2, :, cols, high, :], side_in.at[0, 2], sem.at[OPEN_S], sem.at[OPEN_SIDE],
               (tm, gx, north)),
        remote(state.at[2, :, cols, low, :], side_in.at[1, 2], sem.at[OPEN_S], sem.at[OPEN_SIDE + 1],
               (tm, gx, south)),
    ]
    passed = remote(state.at[1, :, cols, pl.ds(BASE, ROWS), :], prev, sem.at[PASS_S], sem.at[PASS_R], (after, gx, gy))
    for i in range(8):
        @pl.when(earlier[i] == 1)
        def _(i=i):
            halo[i].start()
    for i in range(8):
        @pl.when(earlier[i] == 0)
        def _(i=i):
            pl.semaphore_wait(ready.at[i], 1)
            halo[i].start()

    @pl.when(last)
    def _():
        for copy in opening:
            copy.start()

    later_count = 4 - sum(earlier[8:])

    @pl.when(later_count > 0)
    def _():
        pl.semaphore_wait(ready.at[8], later_count)

    passed.start()

    def await_bytes(ref, i):
        pltpu.make_async_copy(ref, ref, sem.at[i]).wait()

    halo_bytes, y_bytes = state.at[:, :, 0, pl.ds(0, ROWS), :], relay.at[0, 0]
    side_bytes = powers.at[:, 0, 0, 0, pl.ds(0, 2 * HALO), :]
    opening_bytes, opening_side = state.at[2, :, cols, pl.ds(0, 2 * HALO), :], state.at[2, :, cols, pl.ds(0, HALO), :]

    late = jnp.minimum(gy, 1) * jnp.minimum(n_gy - 1 - gy, 1)

    def await_side(side):
        await_bytes(side_bytes, HALO_SIDE + side)

        @pl.when(last)
        def _():
            await_bytes(opening_side, OPEN_SIDE + side)

        state[:, :, cols, pl.ds(pl.multiple_of(EDGE + (HALO + ROWS) * side, 8), HALO), :] = side_in[side]

    row = (gy * ROWS - HALO + n_gy * ROWS + lax.broadcasted_iota(jnp.int32, (TALL, 128), 0)) % (n_gy * ROWS)
    latitude = coriolis_mean + coriolis_slope * ((row.astype(F32) + 0.5) / (n_gy * ROWS) - 0.5)
    rotation[...] = latitude * (1.0 / courant)

    def spread_edges(start, count):
        here = pl.ds(pl.multiple_of(start, 8), count)
        there = pl.ds(pl.multiple_of(EDGE + start, 8), count)
        for s in range(3):
            for f in range(3):
                spot = 8 * (3 * s + f)
                packed = edge_r[here, :]
                right = pltpu.roll(packed, (128 - spot) % 128, 1) if spot else packed
                left = pltpu.roll(edge_l[here, :], 120 - spot, 1)
                state[s, f, 2, there, :] = jnp.where(lane_id[:count] < 64, right, left)

    def dx(tiles):
        ahead = [pltpu.roll(t, 127, 1) for t in tiles]
        behind = [pltpu.roll(t, 1, 1) for t in tiles]
        lane = lane_id[: tiles[0].shape[0]]
        return [jnp.where(lane == 127, ahead[(l + 1) % 3], ahead[l]) - jnp.where(lane == 0, behind[(l + 2) % 3], behind[l])
                for l in range(3)]

    def all_powers(start, count, block_start, block_count):
        def at(first_row, rows):
            begin = pl.multiple_of(EDGE + first_row, 8)
            return pl.ds(begin, rows), pl.ds(begin + 1, rows), pl.ds(begin - 1, rows)

        tall, above, below = at(start, count)
        turns = pl.ds(pl.multiple_of(start, 8), count)

        def start_fields(s, carry):
            h = [state[s, 0, l, tall, :] for l in range(3)]
            u = [state[s, 1, l, tall, :] for l in range(3)]
            v = [state[s, 2, l, tall, :] for l in range(3)]
            turn = rotation[turns, :]
            flux = dx([u[l] + h[l] * u[l] for l in range(3)])
            slope_h, slope_u, slope_v = dx(h), dx(u), dx(v)
            for l in range(3):
                (ha, hb), (ua, ub), (va, vb) = [(state[s, f, l, above, :], state[s, f, l, below, :]) for f in range(3)]
                powers[0, s, 0, l, tall, :] = h[l] + courant * (flux[l] + ((va + ha * va) - (vb + hb * vb)))
                powers[0, s, 1, l, tall, :] = u[l] + courant * (
                    slope_h[l] - turn * v[l] + (u[l] * slope_u[l] + v[l] * (ua - ub)))
                powers[0, s, 2, l, tall, :] = v[l] + courant * (
                    (ha - hb) + turn * u[l] + (u[l] * slope_v[l] + v[l] * (va - vb)))
            return carry

        lax.fori_loop(0, 2, start_fields, 0)

        slot = jnp.where(last, 2, 1)
        factor = jnp.where(last, -WRAPS, -1.0).astype(F32)
        for f in range(3):
            for l in range(3):
                powers[0, 2, f, l, tall, :] = factor * state[slot, f, l, tall, :]
                powers[0, 1, f, l, tall, :] = powers[0, 1, f, l, tall, :] - state[0, f, l, tall, :]

        def apply(m, rows, turns, tiles):
            here, up, down = rows
            for q in range(3):
                h = [powers[m, q, 0, l, here, :] for l in range(3)]
                u = [powers[m, q, 1, l, here, :] for l in range(3)]
                slope_h, slope_u = dx(h), dx(u)
                turn = rotation[turns, :]
                for l in range(tiles):
                    ha, hb = powers[m, q, 0, l, up, :], powers[m, q, 0, l, down, :]
                    va, vb = powers[m, q, 2, l, up, :], powers[m, q, 2, l, down, :]
                    v = powers[m, q, 2, l, here, :]
                    powers[m + 1, q, 0, l, here, :] = slope_u[l] + (va - vb)
                    powers[m + 1, q, 1, l, here, :] = slope_h[l] - turn * v
                    powers[m + 1, q, 2, l, here, :] = (ha - hb) + turn * u[l]

        def next_power(m, carry):
            apply(m, (tall, above, below), turns, 3)
            return carry

        lax.fori_loop(0, CHEB - 1, next_power, 0)
        apply(CHEB - 1, at(HALO + block_start, block_count), pl.ds(pl.multiple_of(HALO + block_start, 8), block_count), 2)

    most, rest = REST * (1 - late), MOST * late
    await_bytes(y_bytes, HALO_Y)
    await_side(1 - late)
    spread_edges(HALO * (1 - late), TALL - HALO)
    all_powers(HALO * (1 - late), TALL - HALO, most, MOST)

    block = pl.ds(BASE, ROWS)

    class Part:
        def __init__(self, start, count):
            self.rows = pl.ds(pl.multiple_of(start, 8), count)
            self.source = pl.ds(pl.multiple_of(BASE + start, 8), count)
            self.size = pl.ds(0, count)

    large, small, whole = Part(most, MOST), Part(rest, REST), Part(0, ROWS)

    def mix(part, f, wanted):
        def body(l, carry):
            totals = [None] * len(wanted)
            for q in range(3):
                for m in range(CHEB + 1):
                    value = powers[m, q, f, l, part.source, :]
                    for i, (delta, p, _, _) in enumerate(wanted):
                        term = weight(delta, p, q, m) * value
                        totals[i] = term if totals[i] is None else totals[i] + term
            for (delta, p, ref, index), total in zip(wanted, totals, strict=True):
                if delta:
                    total = total * jnp.where(tm + delta >= n_tm, circulant, 1.0).astype(F32)
                ref[(*index, l, part.rows, slice(None))] = total
            return carry
        lax.fori_loop(0, 2, body, 0)

    def both_steps(delta, ref, *index):
        return [(delta, p, ref, (*index, p)) for p in range(2)]

    def odd_delta(seat, place):
        return (2 * place + 1 - 2 * seat) % 8

    def for_partner(part, f, places):
        for seat in range(2):
            @pl.when(core == seat)
            def _(seat=seat):
                mix(part, f, [w for place in places for w in both_steps(odd_delta(seat, place), cross, place, f)])

    def send_across(part, f, place, i):
        remote(cross.at[place, f, :, :, part.rows, :], crossed.at[place, f, :, :, part.rows, :], sem.at[CROSS_S], sem.at[i],
               (partner, gx, gy)).start()

    up, down = (chip_up, gx, gy), (chip_down, gx, gy)

    def send_ring(i, side, src, dst):
        remote(src, dst, sem.at[RING_S], sem.at[i], down if side else up).start()

    def add_into(part, f, place, i, other):
        own[i, f, :, :, part.rows, :] = own[i, f, :, :, part.rows, :] + crossed[other, f, :, :, part.rows, :]

    def send_far(part, f, i):
        for side in range(2):
            send_ring(i, side, own.at[0, f, side, :, part.rows, :], relay.at[side, f, :, part.rows, :])

    def send_near(part, f, i):
        for side in range(2):
            send_ring(i, side, own.at[1 + side, f, 1 - side, :, part.rows, :], near_a.at[side, f, :, part.rows, :])

    def send_relayed(part, f, i):
        for side in range(2):
            send_ring(i, side, own.at[1 + side, f, side, :, part.rows, :], near_b.at[side, f, :, part.rows, :])

    def add_relayed(part, f):
        for side in range(2):
            own[1 + side, f, side, :, part.rows, :] = (
                own[1 + side, f, side, :, part.rows, :] + relay[side, f, :, part.rows, :])

    def each_field(body):
        def step(f, carry):
            body(f)
            return carry
        lax.fori_loop(0, 3, step, 0)

    def far_odd(f):
        for_partner(large, f, (2,))
        send_across(large, f, 2, CROSS_FAR + f)

    def far_out(f):
        for_partner(large, f, (1, 3))
        send_across(large, f, 1, CROSS_NEAR + f)
        send_across(large, f, 3, CROSS_NEAR + f)
        await_bytes(crossed.at[2, f, :, :, large.size, :], CROSS_FAR + f)
        add_into(large, f, 2, 0, 2)
        send_far(large, f, RING_FAR + f)

    def near_out(f):
        mix(large, f, both_steps(2, own, 1, f) + both_steps(6, own, 2, f))
        await_bytes(crossed.at[pl.ds(0, 2), f, :, :, large.size, :], CROSS_NEAR + f)
        add_into(large, f, 1, 1, 1)
        add_into(large, f, 3, 2, 3)
        send_near(large, f, RING_END + f)

    def relay_out(f):
        await_bytes(relay.at[:, f, :, large.size, :], RING_FAR + f)
        add_relayed(large, f)
        send_relayed(large, f, RING_END + f)

    def here_odd(f):
        for_partner(whole, f, (0,))
        send_across(whole, f, 0, CROSS_OWN)

    each_field(far_odd)
    each_field(lambda f: mix(large, f, both_steps(4, own, 0, f)))
    each_field(far_out)

    await_side(late)
    spread_edges((HALO + ROWS) * late, HALO)
    all_powers(ROWS * late, 2 * HALO, rest, REST)

    fields = slice(None)
    each_field(lambda f: for_partner(small, f, (2,)))
    send_across(small, fields, 2, CROSS_FAR + 3)
    each_field(near_out)
    each_field(lambda f: mix(small, f, both_steps(4, own, 0, f)))
    await_bytes(crossed.at[2, :, :, :, small.size, :], CROSS_FAR + 3)
    add_into(small, fields, 2, 0, 2)
    send_far(small, fields, RING_FAR + 3)
    each_field(lambda f: for_partner(small, f, (1, 3)))
    send_across(small, fields, 1, CROSS_NEAR + 3)
    send_across(small, fields, 3, CROSS_NEAR + 3)
    each_field(lambda f: mix(small, f, both_steps(2, own, 1, f) + both_steps(6, own, 2, f)))
    each_field(relay_out)
    await_bytes(crossed.at[pl.ds(0, 2), :, :, :, small.size, :], CROSS_NEAR + 3)
    add_into(small, fields, 1, 1, 1)
    add_into(small, fields, 3, 2, 3)
    send_near(small, fields, RING_END + 3)
    each_field(here_odd)
    await_bytes(relay.at[:, :, :, small.size, :], RING_FAR + 3)
    add_relayed(small, fields)
    send_relayed(small, fields, RING_END + 3)
    each_field(lambda f: mix(whole, f, both_steps(0, own, 3, f)))

    await_bytes(prev, PASS_R)
    await_bytes(crossed.at[0], CROSS_OWN)
    for f in range(3):
        for l in range(2):
            before_first = jnp.where(tm == 0, state[2, f, l, block, :], prev[f, l])
            res_buf[0, f, l] = powers[0, 0, f, l, block, :] - before_first
            res_buf[1, f, l] = powers[0, 1, f, l, block, :]
            for p in range(2):
                out_buf[p, f, l] = state[p, f, l, block, :] - (own[3, f, p, l] + crossed[0, f, p, l])

    await_bytes(halo_bytes, HALO_S)

    @pl.when(last)
    def _():
        await_bytes(opening_bytes, OPEN_S)

    await_bytes(prev, PASS_S)
    await_bytes(cross, CROSS_S)

    def finish(part, f):
        rows = part.rows
        for p in range(2):
            out_buf[p, f, :, rows, :] = out_buf[p, f, :, rows, :] - (
                near_b[p, f, :, rows, :] + near_a[1 - p, f, :, rows, :])

    def finish_large(f):
        await_bytes(own.at[pl.ds(0, 2), f, :, :, large.size, :], RING_END + f)
        finish(large, f)

    each_field(finish_large)
    await_bytes(own.at[pl.ds(0, 2), :, :, :, small.size, :], RING_END + 3)
    finish(small, fields)
    await_bytes(own.at[pl.ds(0, 3)], RING_S)


def put_out(upd_in, res_in, upd_out, res_out, sem):
    copies = []
    for l in range(2):
        columns = pl.ds(128 * l, 128)
        copies.append(pltpu.make_async_copy(upd_in.at[:, :, l], upd_out.at[:, :, :, columns], sem.at[l]))
        copies.append(pltpu.make_async_copy(res_in.at[:, :, l], res_out.at[:, :, :, columns], sem.at[2 + l]))
    for copy in copies:
        copy.start()
    for copy in copies:
        copy.wait()


def shards(trajectory, initial):
    whole = jax.ShapeDtypeStruct(trajectory.shape, F32)
    anywhere = pl.BlockSpec(memory_space=pl.ANY)
    slow = pl.BlockSpec(memory_space=pltpu.HBM)
    fast = pl.BlockSpec(memory_space=pltpu.VMEM)
    dma = pltpu.SemaphoreType.DMA
    tiles = pltpu.VMEM((2, 3, 2, ROWS, 128), F32)
    updated, residual = pl.pallas_call(
        kernel,
        out_shape=(tiles, tiles),
        in_specs=[slow, slow],
        out_specs=(fast, fast),
        scratch_shapes=[
            pltpu.VMEM((3, 3, 3, DEEP, 128), F32),
            pltpu.VMEM((CHEB + 1, 3, 3, 3, DEEP, 128), F32),
            pltpu.VMEM((TALL, 128), F32),
            pltpu.VMEM((3, 2, ROWS, 128), F32),
            pltpu.VMEM((ROWS, 128), F32),
            pltpu.VMEM((ROWS, 128), F32),
            pltpu.VMEM((TALL, 128), F32),
            pltpu.VMEM((TALL, 128), F32),
            pltpu.VMEM((2, 3, 3, 2, HALO, 128), F32),
            pltpu.VMEM((4, 3, 2, 2, ROWS, 128), F32),
            pltpu.VMEM((4, 3, 2, 2, ROWS, 128), F32),
            pltpu.VMEM((4, 3, 2, 2, ROWS, 128), F32),
            pltpu.VMEM((2, 3, 2, ROWS, 128), F32),
            pltpu.VMEM((2, 3, 2, ROWS, 128), F32),
            pltpu.VMEM((2, 3, 2, ROWS, 128), F32),
            pltpu.SemaphoreType.REGULAR((9,)),
            dma((N_SEM,)),
        ],
        compiler_params=pltpu.CompilerParams(collective_id=0, has_side_effects=True),
        name="paradiag",
    )(trajectory, initial)
    return pl.pallas_call(
        put_out,
        out_shape=(whole, whole),
        in_specs=[anywhere, anywhere],
        out_specs=(anywhere, anywhere),
        scratch_shapes=[dma((4,))],
        compiler_params=pltpu.CompilerParams(vmem_limit_bytes=4 << 20),
        name="put_out",
    )(updated, residual)


def solution(mesh):
    in_specs = (P("tm", None, "gy", "gx"), P(None, "gy", "gx"))
    out_specs = (P("tm", None, "gy", "gx"), P("tm", None, "gy", "gx"))
    return jax.shard_map(shards, mesh=mesh, in_specs=in_specs, out_specs=out_specs, check_vma=False)
```

```python
import math

import jax
import jax.numpy as jnp
import numpy as np
from jax import lax
from jax.experimental import pallas as pl
from jax.experimental.pallas import tpu as pltpu
from jax.sharding import PartitionSpec as P

MESH = pl.DeviceIdType.MESH
F32 = jnp.float32

CHEB = 6
STEPS = 16
courant = 1.5
coriolis_mean = 0.3
coriolis_slope = 0.4
circulant = 0.1
spectrum_edge = 5.0

HALO = 8
ROWS = 32
TALL = ROWS + 2 * HALO
EDGE = 8
BASE = EDGE + HALO
DEEP = TALL + 2 * EDGE
WRAPS = 1.0 / circulant
OPPOSITE = (1, 0, 5, 6, 7, 2, 3, 4, 8, 8, 8, 8)
MOST, REST = 24, 8
(LOAD, HALO_S, HALO_Y, HALO_SIDE, OPEN_S, OPEN_SIDE, PASS_S, PASS_R, CROSS_S, RING_S, CROSS_FAR, CROSS_NEAR, CROSS_OWN, RING_FAR,
 RING_END, N_SEM) = (0, 1, 2, 3, 5, 6, 8, 9, 10, 11, 12, 16, 20, 21, 25, 29)


def power_table():
    beta = circulant ** (1.0 / STEPS)
    solved = np.zeros((STEPS, CHEB + 1), complex)
    for k in range(STEPS):
        theta = 2.0 * np.pi * k / STEPS
        shift = 1.0 - beta * np.cos(theta) + 1j * beta * np.sin(theta)
        edge = 1j * spectrum_edge
        sigma = shift / edge
        rho_old = 1.0 / sigma
        one = np.zeros(CHEB + 2, complex)
        one[0] = 1.0
        update = one / shift
        total = update.copy()
        for _ in range(CHEB):
            misfit = one - (shift * total + np.roll(total, 1))
            rho_new = 1.0 / (2.0 * sigma - rho_old)
            update = rho_new * rho_old * update + 2.0 * rho_new / edge * misfit
            total = total + update
            rho_old = rho_new
        solved[k] = total[: CHEB + 1]
    turns = np.exp(2j * np.pi / STEPS * np.outer(np.arange(STEPS), np.arange(STEPS)))
    table = (turns @ solved).real / STEPS
    return table * courant ** np.arange(CHEB + 1)


TABLE = power_table()


def weight(delta, p, q, m):
    difference = 2 * delta + p - q
    return float(circulant ** (-difference / STEPS) * TABLE[difference % STEPS, m])


def kernel(
    traj, init, out_buf, res_buf,
    state, powers, rotation, prev, strip_l, strip_r, edge_l, edge_r,
    side_in, cross, crossed, own, relay, near_a, near_b,
    ready, sem,
):
    tm, gx, gy = lax.axis_index("tm"), lax.axis_index("gx"), lax.axis_index("gy")
    n_tm, n_gx, n_gy = lax.axis_size("tm"), lax.axis_size("gx"), lax.axis_size("gy")
    core = lax.rem(tm, 2)
    east, west = lax.rem(gx + 1, n_gx), lax.rem(gx + n_gx - 1, n_gx)
    north, south = lax.rem(gy + 1, n_gy), lax.rem(gy + n_gy - 1, n_gy)
    after, before = lax.rem(tm + 1, n_tm), lax.rem(tm + n_tm - 1, n_tm)
    chip_up, chip_down = lax.rem(tm + 2, n_tm), lax.rem(tm + n_tm - 2, n_tm)
    partner = tm + 1 - 2 * core
    last = tm == n_tm - 1

    loads = []
    for lane in range(2):
        columns = pl.ds(128 * lane, 128)
        loads.append(pltpu.make_async_copy(
            traj.at[:, :, :, columns], state.at[pl.ds(0, 2), :, lane, pl.ds(BASE, ROWS), :], sem.at[LOAD]))
        loads.append(pltpu.make_async_copy(
            init.at[:, :, columns], state.at[2, :, lane, pl.ds(BASE, ROWS), :], sem.at[LOAD]))
    for load in loads:
        load.start()
    loaded = state.at[:, :, pl.ds(0, 2), pl.ds(BASE, ROWS), :]

    def arrival(t, x, y):
        by_z = jnp.minimum(2 * y + 2 * jnp.minimum(y, 1), 11)
        return (t // 2 + x + by_z + 1 - t % 2) * 256 + t * 32 + x * 8 + y

    across = jnp.where(core == 1, after, before)
    peers = [(tm, east, gy), (tm, west, gy), (tm, gx, north), (tm, east, north), (tm, west, north),
             (tm, gx, south), (tm, west, south), (tm, east, south),
             (partner, gx, gy), (chip_up, gx, gy), (chip_down, gx, gy), (across, gx, gy)]
    mine = arrival(tm, gx, gy)
    earlier = [(arrival(*peer) < mine).astype(jnp.int32) for peer in peers]

    barrier = pltpu.get_barrier_semaphore()
    for peer, sooner in zip(peers, earlier, strict=True):
        @pl.when(sooner == 0)
        def _(peer=peer):
            pl.semaphore_signal(barrier, inc=1, device_id=peer, device_id_type=MESH)

    sooner_count = sum(earlier)

    @pl.when(sooner_count > 0)
    def _():
        pl.semaphore_wait(barrier, sooner_count)

    for i, (peer, sooner) in enumerate(zip(peers, earlier, strict=True)):
        @pl.when(sooner == 1)
        def _(i=i, peer=peer):
            pl.semaphore_signal(ready.at[OPPOSITE[i]], inc=1, device_id=peer, device_id_type=MESH)

    pltpu.make_async_copy(loaded, loaded, sem.at[LOAD]).wait()

    lane_id = lax.broadcasted_iota(jnp.int32, (TALL, 128), 1)
    packed_l = jnp.zeros((ROWS, 128), F32)
    packed_r = jnp.zeros((ROWS, 128), F32)
    for s in range(3):
        for f in range(3):
            spot = 8 * (3 * s + f)
            here = (lane_id[:ROWS] >= spot) & (lane_id[:ROWS] < spot + 8)
            left = state[s, f, 0, pl.ds(BASE, ROWS), :]
            right = state[s, f, 1, pl.ds(BASE, ROWS), :]
            packed_l = jnp.where(here, pltpu.roll(left, spot, 1) if spot else left, packed_l)
            packed_r = jnp.where(here, pltpu.roll(right, spot + 8, 1), packed_r)
    strip_l[...] = packed_l
    strip_r[...] = packed_r

    def remote(src, dst, send, recv, peer):
        return pltpu.make_async_remote_copy(
            src_ref=src, dst_ref=dst, send_sem=send, recv_sem=recv, device_id=peer, device_id_type=MESH)

    top, bottom, low, high = pl.ds(0, HALO), pl.ds(ROWS - HALO, HALO), pl.ds(BASE, HALO), pl.ds(EDGE + ROWS, HALO)
    first, final = pl.ds(0, HALO), pl.ds(HALO + ROWS, HALO)
    both, cols = pl.ds(0, 2), pl.ds(0, 2)
    middle = pl.ds(HALO, ROWS)
    sides = [
        (strip_r, edge_l.at[middle]),
        (strip_l, edge_r.at[middle]),
        (state.at[both, :, cols, high, :], side_in.at[0, both]),
        (strip_r.at[bottom], edge_l.at[first]),
        (strip_l.at[bottom], edge_r.at[first]),
        (state.at[both, :, cols, low, :], side_in.at[1, both]),
        (strip_l.at[top], edge_r.at[final]),
        (strip_r.at[top], edge_l.at[final]),
    ]
    seats = (HALO_Y, HALO_Y, HALO_SIDE, HALO_SIDE, HALO_SIDE, HALO_SIDE + 1, HALO_SIDE + 1, HALO_SIDE + 1)
    halo = [remote(src, dst, sem.at[HALO_S], sem.at[seats[i]], peers[i]) for i, (src, dst) in enumerate(sides)]
    opening = [
        remote(state.at[2, :, cols, high, :], side_in.at[0, 2], sem.at[OPEN_S], sem.at[OPEN_SIDE],
               (tm, gx, north)),
        remote(state.at[2, :, cols, low, :], side_in.at[1, 2], sem.at[OPEN_S], sem.at[OPEN_SIDE + 1],
               (tm, gx, south)),
    ]
    passed = remote(state.at[1, :, cols, pl.ds(BASE, ROWS), :], prev, sem.at[PASS_S], sem.at[PASS_R], (after, gx, gy))
    for i in range(8):
        @pl.when(earlier[i] == 1)
        def _(i=i):
            halo[i].start()
    for i in range(8):
        @pl.when(earlier[i] == 0)
        def _(i=i):
            pl.semaphore_wait(ready.at[i], 1)
            halo[i].start()

    @pl.when(last)
    def _():
        for copy in opening:
            copy.start()

    later_count = 4 - sum(earlier[8:])

    @pl.when(later_count > 0)
    def _():
        pl.semaphore_wait(ready.at[8], later_count)

    passed.start()

    def await_bytes(ref, i):
        pltpu.make_async_copy(ref, ref, sem.at[i]).wait()

    halo_bytes, y_bytes = state.at[:, :, 0, pl.ds(0, ROWS), :], relay.at[0, 0]
    side_bytes = powers.at[:, 0, 0, 0, pl.ds(0, 2 * HALO), :]
    opening_bytes, opening_side = state.at[2, :, cols, pl.ds(0, 2 * HALO), :], state.at[2, :, cols, pl.ds(0, HALO), :]

    late = jnp.minimum(gy, 1) * jnp.minimum(n_gy - 1 - gy, 1)

    def await_side(side):
        await_bytes(side_bytes, HALO_SIDE + side)

        @pl.when(last)
        def _():
            await_bytes(opening_side, OPEN_SIDE + side)

        state[:, :, cols, pl.ds(pl.multiple_of(EDGE + (HALO + ROWS) * side, 8), HALO), :] = side_in[side]

    row = (gy * ROWS - HALO + n_gy * ROWS + lax.broadcasted_iota(jnp.int32, (TALL, 128), 0)) % (n_gy * ROWS)
    latitude = coriolis_mean + coriolis_slope * ((row.astype(F32) + 0.5) / (n_gy * ROWS) - 0.5)
    rotation[...] = latitude * (1.0 / courant)

    def spread_edges(start, count):
        here = pl.ds(pl.multiple_of(start, 8), count)
        there = pl.ds(pl.multiple_of(EDGE + start, 8), count)
        for s in range(3):
            for f in range(3):
                spot = 8 * (3 * s + f)
                packed = edge_r[here, :]
                right = pltpu.roll(packed, (128 - spot) % 128, 1) if spot else packed
                left = pltpu.roll(edge_l[here, :], 120 - spot, 1)
                state[s, f, 2, there, :] = jnp.where(lane_id[:count] < 64, right, left)

    def dx(tiles):
        ahead = [pltpu.roll(t, 127, 1) for t in tiles]
        behind = [pltpu.roll(t, 1, 1) for t in tiles]
        lane = lane_id[: tiles[0].shape[0]]
        return [jnp.where(lane == 127, ahead[(l + 1) % 3], ahead[l]) - jnp.where(lane == 0, behind[(l + 2) % 3], behind[l])
                for l in range(3)]

    def all_powers(start, count, block_start, block_count):
        def at(first_row, rows):
            begin = pl.multiple_of(EDGE + first_row, 8)
            return pl.ds(begin, rows), pl.ds(begin + 1, rows), pl.ds(begin - 1, rows)

        tall, above, below = at(start, count)
        turns = pl.ds(pl.multiple_of(start, 8), count)

        def start_fields(s, carry):
            h = [state[s, 0, l, tall, :] for l in range(3)]
            u = [state[s, 1, l, tall, :] for l in range(3)]
            v = [state[s, 2, l, tall, :] for l in range(3)]
            turn = rotation[turns, :]
            flux = dx([u[l] + h[l] * u[l] for l in range(3)])
            slope_h, slope_u, slope_v = dx(h), dx(u), dx(v)
            for l in range(3):
                (ha, hb), (ua, ub), (va, vb) = [(state[s, f, l, above, :], state[s, f, l, below, :]) for f in range(3)]
                powers[0, s, 0, l, tall, :] = h[l] + courant * (flux[l] + ((va + ha * va) - (vb + hb * vb)))
                powers[0, s, 1, l, tall, :] = u[l] + courant * (
                    slope_h[l] - turn * v[l] + (u[l] * slope_u[l] + v[l] * (ua - ub)))
                powers[0, s, 2, l, tall, :] = v[l] + courant * (
                    (ha - hb) + turn * u[l] + (u[l] * slope_v[l] + v[l] * (va - vb)))
            return carry

        for s in range(2):
            start_fields(s, 0)

        slot = jnp.where(last, 2, 1)
        factor = jnp.where(last, -WRAPS, -1.0).astype(F32)
        for f in range(3):
            for l in range(3):
                powers[0, 2, f, l, tall, :] = factor * state[slot, f, l, tall, :]
                powers[0, 1, f, l, tall, :] = powers[0, 1, f, l, tall, :] - state[0, f, l, tall, :]

        def apply(m, rows, turns, tiles):
            here, up, down = rows
            for q in range(3):
                h = [powers[m, q, 0, l, here, :] for l in range(3)]
                u = [powers[m, q, 1, l, here, :] for l in range(3)]
                slope_h, slope_u = dx(h), dx(u)
                turn = rotation[turns, :]
                for l in range(tiles):
                    ha, hb = powers[m, q, 0, l, up, :], powers[m, q, 0, l, down, :]
                    va, vb = powers[m, q, 2, l, up, :], powers[m, q, 2, l, down, :]
                    v = powers[m, q, 2, l, here, :]
                    powers[m + 1, q, 0, l, here, :] = slope_u[l] + (va - vb)
                    powers[m + 1, q, 1, l, here, :] = slope_h[l] - turn * v
                    powers[m + 1, q, 2, l, here, :] = (ha - hb) + turn * u[l]

        def next_power(m, carry):
            apply(m, (tall, above, below), turns, 3)
            return carry

        for m in range(CHEB - 1):
            next_power(m, 0)
        apply(CHEB - 1, at(HALO + block_start, block_count), pl.ds(pl.multiple_of(HALO + block_start, 8), block_count), 2)

    most, rest = REST * (1 - late), MOST * late
    await_bytes(y_bytes, HALO_Y)
    await_side(1 - late)
    spread_edges(HALO * (1 - late), TALL - HALO)
    all_powers(HALO * (1 - late), TALL - HALO, most, MOST)

    block = pl.ds(BASE, ROWS)

    class Part:
        def __init__(self, start, count):
            self.rows = pl.ds(pl.multiple_of(start, 8), count)
            self.source = pl.ds(pl.multiple_of(BASE + start, 8), count)
            self.size = pl.ds(0, count)

    large, small, whole = Part(most, MOST), Part(rest, REST), Part(0, ROWS)

    def mix(part, f, wanted):
        def body(l, carry):
            totals = [None] * len(wanted)
            for q in range(3):
                for m in range(CHEB + 1):
                    value = powers[m, q, f, l, part.source, :]
                    for i, (delta, p, _, _) in enumerate(wanted):
                        term = weight(delta, p, q, m) * value
                        totals[i] = term if totals[i] is None else totals[i] + term
            for (delta, p, ref, index), total in zip(wanted, totals, strict=True):
                if delta:
                    total = total * jnp.where(tm + delta >= n_tm, circulant, 1.0).astype(F32)
                ref[(*index, l, part.rows, slice(None))] = total
            return carry
        for l in range(2):
            body(l, 0)

    def both_steps(delta, ref, *index):
        return [(delta, p, ref, (*index, p)) for p in range(2)]

    def odd_delta(seat, place):
        return (2 * place + 1 - 2 * seat) % 8

    def for_partner(part, f, places):
        for seat in range(2):
            @pl.when(core == seat)
            def _(seat=seat):
                mix(part, f, [w for place in places for w in both_steps(odd_delta(seat, place), cross, place, f)])

    def send_across(part, f, place, i):
        remote(cross.at[place, f, :, :, part.rows, :], crossed.at[place, f, :, :, part.rows, :], sem.at[CROSS_S], sem.at[i],
               (partner, gx, gy)).start()

    up, down = (chip_up, gx, gy), (chip_down, gx, gy)

    def send_ring(i, side, src, dst):
        remote(src, dst, sem.at[RING_S], sem.at[i], down if side else up).start()

    def add_into(part, f, place, i, other):
        own[i, f, :, :, part.rows, :] = own[i, f, :, :, part.rows, :] + crossed[other, f, :, :, part.rows, :]

    def send_far(part, f, i):
        for side in range(2):
            send_ring(i, side, own.at[0, f, side, :, part.rows, :], relay.at[side, f, :, part.rows, :])

    def send_near(part, f, i):
        for side in range(2):
            send_ring(i, side, own.at[1 + side, f, 1 - side, :, part.rows, :], near_a.at[side, f, :, part.rows, :])

    def send_relayed(part, f, i):
        for side in range(2):
            send_ring(i, side, own.at[1 + side, f, side, :, part.rows, :], near_b.at[side, f, :, part.rows, :])

    def add_relayed(part, f):
        for side in range(2):
            own[1 + side, f, side, :, part.rows, :] = (
                own[1 + side, f, side, :, part.rows, :] + relay[side, f, :, part.rows, :])

    def each_field(body):
        def step(f, carry):
            body(f)
            return carry
        lax.fori_loop(0, 3, step, 0)

    def far_odd(f):
        for_partner(large, f, (2,))
        send_across(large, f, 2, CROSS_FAR + f)

    def far_out(f):
        for_partner(large, f, (1, 3))
        send_across(large, f, 1, CROSS_NEAR + f)
        send_across(large, f, 3, CROSS_NEAR + f)
        await_bytes(crossed.at[2, f, :, :, large.size, :], CROSS_FAR + f)
        add_into(large, f, 2, 0, 2)
        send_far(large, f, RING_FAR + f)

    def near_out(f):
        mix(large, f, both_steps(2, own, 1, f) + both_steps(6, own, 2, f))
        await_bytes(crossed.at[pl.ds(0, 2), f, :, :, large.size, :], CROSS_NEAR + f)
        add_into(large, f, 1, 1, 1)
        add_into(large, f, 3, 2, 3)
        send_near(large, f, RING_END + f)

    def relay_out(f):
        await_bytes(relay.at[:, f, :, large.size, :], RING_FAR + f)
        add_relayed(large, f)
        send_relayed(large, f, RING_END + f)

    def here_odd(f):
        for_partner(whole, f, (0,))
        send_across(whole, f, 0, CROSS_OWN)

    each_field(far_odd)
    each_field(lambda f: mix(large, f, both_steps(4, own, 0, f)))
    each_field(far_out)

    await_side(late)
    spread_edges((HALO + ROWS) * late, HALO)
    all_powers(ROWS * late, 2 * HALO, rest, REST)

    fields = slice(None)
    each_field(lambda f: for_partner(small, f, (2,)))
    send_across(small, fields, 2, CROSS_FAR + 3)
    each_field(near_out)
    each_field(lambda f: mix(small, f, both_steps(4, own, 0, f)))
    await_bytes(crossed.at[2, :, :, :, small.size, :], CROSS_FAR + 3)
    add_into(small, fields, 2, 0, 2)
    send_far(small, fields, RING_FAR + 3)
    each_field(lambda f: for_partner(small, f, (1, 3)))
    send_across(small, fields, 1, CROSS_NEAR + 3)
    send_across(small, fields, 3, CROSS_NEAR + 3)
    each_field(lambda f: mix(small, f, both_steps(2, own, 1, f) + both_steps(6, own, 2, f)))
    each_field(relay_out)
    await_bytes(crossed.at[pl.ds(0, 2), :, :, :, small.size, :], CROSS_NEAR + 3)
    add_into(small, fields, 1, 1, 1)
    add_into(small, fields, 3, 2, 3)
    send_near(small, fields, RING_END + 3)
    each_field(here_odd)
    await_bytes(relay.at[:, :, :, small.size, :], RING_FAR + 3)
    add_relayed(small, fields)
    send_relayed(small, fields, RING_END + 3)
    each_field(lambda f: mix(whole, f, both_steps(0, own, 3, f)))

    await_bytes(prev, PASS_R)
    await_bytes(crossed.at[0], CROSS_OWN)
    for f in range(3):
        for l in range(2):
            before_first = jnp.where(tm == 0, state[2, f, l, block, :], prev[f, l])
            res_buf[0, f, l] = powers[0, 0, f, l, block, :] - before_first
            res_buf[1, f, l] = powers[0, 1, f, l, block, :]
            for p in range(2):
                out_buf[p, f, l] = state[p, f, l, block, :] - (own[3, f, p, l] + crossed[0, f, p, l])

    await_bytes(halo_bytes, HALO_S)

    @pl.when(last)
    def _():
        await_bytes(opening_bytes, OPEN_S)

    await_bytes(prev, PASS_S)
    await_bytes(cross, CROSS_S)

    def finish(part, f):
        rows = part.rows
        for p in range(2):
            out_buf[p, f, :, rows, :] = out_buf[p, f, :, rows, :] - (
                near_b[p, f, :, rows, :] + near_a[1 - p, f, :, rows, :])

    def finish_large(f):
        await_bytes(own.at[pl.ds(0, 2), f, :, :, large.size, :], RING_END + f)
        finish(large, f)

    each_field(finish_large)
    await_bytes(own.at[pl.ds(0, 2), :, :, :, small.size, :], RING_END + 3)
    finish(small, fields)
    await_bytes(own.at[pl.ds(0, 3)], RING_S)


def put_out(upd_in, res_in, upd_out, res_out, sem):
    copies = []
    for l in range(2):
        columns = pl.ds(128 * l, 128)
        copies.append(pltpu.make_async_copy(upd_in.at[:, :, l], upd_out.at[:, :, :, columns], sem.at[l]))
        copies.append(pltpu.make_async_copy(res_in.at[:, :, l], res_out.at[:, :, :, columns], sem.at[2 + l]))
    for copy in copies:
        copy.start()
    for copy in copies:
        copy.wait()


def shards(trajectory, initial):
    whole = jax.ShapeDtypeStruct(trajectory.shape, F32)
    anywhere = pl.BlockSpec(memory_space=pl.ANY)
    slow = pl.BlockSpec(memory_space=pltpu.HBM)
    fast = pl.BlockSpec(memory_space=pltpu.VMEM)
    dma = pltpu.SemaphoreType.DMA
    tiles = pltpu.VMEM((2, 3, 2, ROWS, 128), F32)
    updated, residual = pl.pallas_call(
        kernel,
        out_shape=(tiles, tiles),
        in_specs=[slow, slow],
        out_specs=(fast, fast),
        scratch_shapes=[
            pltpu.VMEM((3, 3, 3, DEEP, 128), F32),
            pltpu.VMEM((CHEB + 1, 3, 3, 3, DEEP, 128), F32),
            pltpu.VMEM((TALL, 128), F32),
            pltpu.VMEM((3, 2, ROWS, 128), F32),
            pltpu.VMEM((ROWS, 128), F32),
            pltpu.VMEM((ROWS, 128), F32),
            pltpu.VMEM((TALL, 128), F32),
            pltpu.VMEM((TALL, 128), F32),
            pltpu.VMEM((2, 3, 3, 2, HALO, 128), F32),
            pltpu.VMEM((4, 3, 2, 2, ROWS, 128), F32),
            pltpu.VMEM((4, 3, 2, 2, ROWS, 128), F32),
            pltpu.VMEM((4, 3, 2, 2, ROWS, 128), F32),
            pltpu.VMEM((2, 3, 2, ROWS, 128), F32),
            pltpu.VMEM((2, 3, 2, ROWS, 128), F32),
            pltpu.VMEM((2, 3, 2, ROWS, 128), F32),
            pltpu.SemaphoreType.REGULAR((9,)),
            dma((N_SEM,)),
        ],
        compiler_params=pltpu.CompilerParams(collective_id=0, has_side_effects=True),
        name="paradiag",
    )(trajectory, initial)
    return pl.pallas_call(
        put_out,
        out_shape=(whole, whole),
        in_specs=[anywhere, anywhere],
        out_specs=(anywhere, anywhere),
        scratch_shapes=[dma((4,))],
        compiler_params=pltpu.CompilerParams(vmem_limit_bytes=4 << 20),
        name="put_out",
    )(updated, residual)


def solution(mesh):
    in_specs = (P("tm", None, "gy", "gx"), P(None, "gy", "gx"))
    out_specs = (P("tm", None, "gy", "gx"), P("tm", None, "gy", "gx"))
    return jax.shard_map(shards, mesh=mesh, in_specs=in_specs, out_specs=out_specs, check_vma=False)
```

```python
import math

import jax
import jax.numpy as jnp
import numpy as np
from jax import lax
from jax.experimental import pallas as pl
from jax.experimental.pallas import tpu as pltpu
from jax.sharding import PartitionSpec as P

MESH = pl.DeviceIdType.MESH
F32 = jnp.float32

CHEB = 6
STEPS = 16
courant = 1.5
coriolis_mean = 0.3
coriolis_slope = 0.4
circulant = 0.1
spectrum_edge = 5.0

HALO = 8
ROWS = 32
TALL = ROWS + 2 * HALO
EDGE = 8
BASE = EDGE + HALO
DEEP = TALL + 2 * EDGE
WRAPS = 1.0 / circulant
OPPOSITE = (1, 0, 5, 6, 7, 2, 3, 4, 8, 8, 8, 8)
MOST, REST = 24, 8
(LOAD, HALO_S, HALO_Y, HALO_SIDE, OPEN_S, OPEN_SIDE, PASS_S, PASS_R, CROSS_S, RING_S, CROSS_FAR, CROSS_NEAR, CROSS_OWN, RING_FAR,
 RING_END, N_SEM) = (0, 1, 2, 3, 5, 6, 8, 9, 10, 11, 12, 16, 20, 21, 25, 26)


def power_table():
    beta = circulant ** (1.0 / STEPS)
    solved = np.zeros((STEPS, CHEB + 1), complex)
    for k in range(STEPS):
        theta = 2.0 * np.pi * k / STEPS
        shift = 1.0 - beta * np.cos(theta) + 1j * beta * np.sin(theta)
        edge = 1j * spectrum_edge
        sigma = shift / edge
        rho_old = 1.0 / sigma
        one = np.zeros(CHEB + 2, complex)
        one[0] = 1.0
        update = one / shift
        total = update.copy()
        for _ in range(CHEB):
            misfit = one - (shift * total + np.roll(total, 1))
            rho_new = 1.0 / (2.0 * sigma - rho_old)
            update = rho_new * rho_old * update + 2.0 * rho_new / edge * misfit
            total = total + update
            rho_old = rho_new
        solved[k] = total[: CHEB + 1]
    turns = np.exp(2j * np.pi / STEPS * np.outer(np.arange(STEPS), np.arange(STEPS)))
    table = (turns @ solved).real / STEPS
    return table * courant ** np.arange(CHEB + 1)


TABLE = power_table()


def weight(delta, p, q, m):
    difference = 2 * delta + p - q
    return float(circulant ** (-difference / STEPS) * TABLE[difference % STEPS, m])


def kernel(
    traj, init, out_buf, res_buf,
    state, powers, rotation, prev, strip_l, strip_r, edge_l, edge_r,
    side_in, cross, crossed, own, relay, near_a, near_b,
    ready, sem,
):
    tm, gx, gy = lax.axis_index("tm"), lax.axis_index("gx"), lax.axis_index("gy")
    n_tm, n_gx, n_gy = lax.axis_size("tm"), lax.axis_size("gx"), lax.axis_size("gy")
    core = lax.rem(tm, 2)
    east, west = lax.rem(gx + 1, n_gx), lax.rem(gx + n_gx - 1, n_gx)
    north, south = lax.rem(gy + 1, n_gy), lax.rem(gy + n_gy - 1, n_gy)
    after, before = lax.rem(tm + 1, n_tm), lax.rem(tm + n_tm - 1, n_tm)
    chip_up, chip_down = lax.rem(tm + 2, n_tm), lax.rem(tm + n_tm - 2, n_tm)
    partner = tm + 1 - 2 * core
    last = tm == n_tm - 1

    loads = []
    for lane in range(2):
        columns = pl.ds(128 * lane, 128)
        loads.append(pltpu.make_async_copy(
            traj.at[:, :, :, columns], state.at[pl.ds(0, 2), :, lane, pl.ds(BASE, ROWS), :], sem.at[LOAD]))
        loads.append(pltpu.make_async_copy(
            init.at[:, :, columns], state.at[2, :, lane, pl.ds(BASE, ROWS), :], sem.at[LOAD]))
    for load in loads:
        load.start()
    loaded = state.at[:, :, pl.ds(0, 2), pl.ds(BASE, ROWS), :]

    across = jnp.where(core == 1, after, before)
    peers = [(tm, east, gy), (tm, west, gy), (tm, gx, north), (tm, east, north), (tm, west, north),
             (tm, gx, south), (tm, west, south), (tm, east, south),
             (partner, gx, gy), (chip_up, gx, gy), (chip_down, gx, gy), (across, gx, gy)]
    chip = lax.div(tm, 2)
    next_chip, prior_chip = lax.rem(chip + 1, n_tm // 2), lax.rem(chip + n_tm // 2 - 1, n_tm // 2)

    def key_t(its_chip, its_core):
        return (its_chip + 1 - its_core) * 256 + (2 * its_chip + its_core) * 32

    def key_z(y):
        return jnp.minimum(2 * y + 2 * jnp.minimum(y, 1), 11) * 256 + y

    mine_t, mine_x, mine_z = key_t(chip, core), gx * 264, key_z(gy)
    east_x, west_x, north_z, south_z = east * 264, west * 264, key_z(north), key_z(south)
    mine = mine_t + mine_x + mine_z
    keys = [mine_t + east_x + mine_z, mine_t + west_x + mine_z, mine_t + mine_x + north_z, mine_t + east_x + north_z,
            mine_t + west_x + north_z, mine_t + mine_x + south_z, mine_t + west_x + south_z, mine_t + east_x + south_z,
            key_t(chip, 1 - core) + mine_x + mine_z, key_t(next_chip, core) + mine_x + mine_z,
            key_t(prior_chip, core) + mine_x + mine_z,
            key_t(jnp.where(core == 1, next_chip, prior_chip), 1 - core) + mine_x + mine_z]
    earlier = [(key < mine).astype(jnp.int32) for key in keys]

    barrier = pltpu.get_barrier_semaphore()
    for peer, sooner in zip(peers, earlier, strict=True):
        @pl.when(sooner == 0)
        def _(peer=peer):
            pl.semaphore_signal(barrier, inc=1, device_id=peer, device_id_type=MESH)

    sooner_count = sum(earlier)

    @pl.when(sooner_count > 0)
    def _():
        pl.semaphore_wait(barrier, sooner_count)

    for i, (peer, sooner) in enumerate(zip(peers, earlier, strict=True)):
        @pl.when(sooner == 1)
        def _(i=i, peer=peer):
            pl.semaphore_signal(ready.at[OPPOSITE[i]], inc=1, device_id=peer, device_id_type=MESH)

    pltpu.make_async_copy(loaded, loaded, sem.at[LOAD]).wait()

    lane_id = lax.broadcasted_iota(jnp.int32, (TALL, 128), 1)
    packed_l = jnp.zeros((ROWS, 128), F32)
    packed_r = jnp.zeros((ROWS, 128), F32)
    for s in range(3):
        for f in range(3):
            spot = 8 * (3 * s + f)
            here = (lane_id[:ROWS] >= spot) & (lane_id[:ROWS] < spot + 8)
            left = state[s, f, 0, pl.ds(BASE, ROWS), :]
            right = state[s, f, 1, pl.ds(BASE, ROWS), :]
            packed_l = jnp.where(here, pltpu.roll(left, spot, 1) if spot else left, packed_l)
            packed_r = jnp.where(here, pltpu.roll(right, spot + 8, 1), packed_r)
    strip_l[...] = packed_l
    strip_r[...] = packed_r

    def remote(src, dst, send, recv, peer):
        return pltpu.make_async_remote_copy(
            src_ref=src, dst_ref=dst, send_sem=send, recv_sem=recv, device_id=peer, device_id_type=MESH)

    top, bottom, low, high = pl.ds(0, HALO), pl.ds(ROWS - HALO, HALO), pl.ds(BASE, HALO), pl.ds(EDGE + ROWS, HALO)
    first, final = pl.ds(0, HALO), pl.ds(HALO + ROWS, HALO)
    both, cols = pl.ds(0, 2), pl.ds(0, 2)
    middle = pl.ds(HALO, ROWS)
    sides = [
        (strip_r, edge_l.at[middle]),
        (strip_l, edge_r.at[middle]),
        (state.at[both, :, cols, high, :], side_in.at[0, both]),
        (strip_r.at[bottom], edge_l.at[first]),
        (strip_l.at[bottom], edge_r.at[first]),
        (state.at[both, :, cols, low, :], side_in.at[1, both]),
        (strip_l.at[top], edge_r.at[final]),
        (strip_r.at[top], edge_l.at[final]),
    ]
    seats = (HALO_Y, HALO_Y, HALO_SIDE, HALO_SIDE, HALO_SIDE, HALO_SIDE + 1, HALO_SIDE + 1, HALO_SIDE + 1)
    halo = [remote(src, dst, sem.at[HALO_S], sem.at[seats[i]], peers[i]) for i, (src, dst) in enumerate(sides)]
    opening = [
        remote(state.at[2, :, cols, high, :], side_in.at[0, 2], sem.at[OPEN_S], sem.at[OPEN_SIDE],
               (tm, gx, north)),
        remote(state.at[2, :, cols, low, :], side_in.at[1, 2], sem.at[OPEN_S], sem.at[OPEN_SIDE + 1],
               (tm, gx, south)),
    ]
    passed = remote(state.at[1, :, cols, pl.ds(BASE, ROWS), :], prev, sem.at[PASS_S], sem.at[PASS_R], (after, gx, gy))
    for i in range(8):
        @pl.when(earlier[i] == 1)
        def _(i=i):
            halo[i].start()
    def send_to_later(i):
        pl.semaphore_wait(ready.at[i], 1)
        halo[i].start()

    at_end = 1 - jnp.minimum(gy, 1)
    for i in range(8):
        @pl.when(earlier[i] + (at_end if i >= 5 else 0) == 0)
        def _(i=i):
            send_to_later(i)

    @pl.when(last)
    def _():
        opening[0].start()

        @pl.when(gy > 0)
        def _():
            opening[1].start()

    later_count = 4 - sum(earlier[8:])

    @pl.when(later_count > 0)
    def _():
        pl.semaphore_wait(ready.at[8], later_count)

    passed.start()

    def await_bytes(ref, i):
        pltpu.make_async_copy(ref, ref, sem.at[i]).wait()

    halo_bytes, y_bytes = state.at[:, :, 0, pl.ds(0, ROWS), :], relay.at[0, 0]
    side_bytes = powers.at[:, 0, 0, 0, pl.ds(0, 2 * HALO), :]
    opening_bytes, opening_side = state.at[2, :, cols, pl.ds(0, 2 * HALO), :], state.at[2, :, cols, pl.ds(0, HALO), :]

    late = jnp.minimum(gy, 1)

    def await_side(side):
        await_bytes(side_bytes, HALO_SIDE + side)

        @pl.when(last)
        def _():
            await_bytes(opening_side, OPEN_SIDE + side)

        state[:, :, cols, pl.ds(pl.multiple_of(EDGE + (HALO + ROWS) * side, 8), HALO), :] = side_in[side]

    row = (gy * ROWS - HALO + n_gy * ROWS + lax.broadcasted_iota(jnp.int32, (TALL, 128), 0)) % (n_gy * ROWS)
    latitude = coriolis_mean + coriolis_slope * ((row.astype(F32) + 0.5) / (n_gy * ROWS) - 0.5)
    rotation[...] = latitude * (1.0 / courant)

    def spread_edges(start, count):
        here = pl.ds(pl.multiple_of(start, 8), count)
        there = pl.ds(pl.multiple_of(EDGE + start, 8), count)
        for s in range(3):
            for f in range(3):
                spot = 8 * (3 * s + f)
                packed = edge_r[here, :]
                right = pltpu.roll(packed, (128 - spot) % 128, 1) if spot else packed
                left = pltpu.roll(edge_l[here, :], 120 - spot, 1)
                state[s, f, 2, there, :] = jnp.where(lane_id[:count] < 64, right, left)

    def dx(tiles):
        ahead = [pltpu.roll(t, 127, 1) for t in tiles]
        behind = [pltpu.roll(t, 1, 1) for t in tiles]
        lane = lane_id[: tiles[0].shape[0]]
        return [jnp.where(lane == 127, ahead[(l + 1) % 3], ahead[l]) - jnp.where(lane == 0, behind[(l + 2) % 3], behind[l])
                for l in range(3)]

    def all_powers(start, count, block_start, block_count):
        def at(first_row, rows):
            begin = pl.multiple_of(EDGE + first_row, 8)
            return pl.ds(begin, rows), pl.ds(begin + 1, rows), pl.ds(begin - 1, rows)

        tall, above, below = at(start, count)
        turns = pl.ds(pl.multiple_of(start, 8), count)

        def start_fields(s, carry):
            h = [state[s, 0, l, tall, :] for l in range(3)]
            u = [state[s, 1, l, tall, :] for l in range(3)]
            v = [state[s, 2, l, tall, :] for l in range(3)]
            turn = rotation[turns, :]
            flux = dx([u[l] + h[l] * u[l] for l in range(3)])
            slope_h, slope_u, slope_v = dx(h), dx(u), dx(v)
            for l in range(3):
                (ha, hb), (ua, ub), (va, vb) = [(state[s, f, l, above, :], state[s, f, l, below, :]) for f in range(3)]
                powers[0, s, 0, l, tall, :] = h[l] + courant * (flux[l] + ((va + ha * va) - (vb + hb * vb)))
                powers[0, s, 1, l, tall, :] = u[l] + courant * (
                    slope_h[l] - turn * v[l] + (u[l] * slope_u[l] + v[l] * (ua - ub)))
                powers[0, s, 2, l, tall, :] = v[l] + courant * (
                    (ha - hb) + turn * u[l] + (u[l] * slope_v[l] + v[l] * (va - vb)))
            return carry

        for s in range(2):
            start_fields(s, 0)

        slot = jnp.where(last, 2, 1)
        factor = jnp.where(last, -WRAPS, -1.0).astype(F32)
        for f in range(3):
            for l in range(3):
                powers[0, 2, f, l, tall, :] = factor * state[slot, f, l, tall, :]
                powers[0, 1, f, l, tall, :] = powers[0, 1, f, l, tall, :] - state[0, f, l, tall, :]

        def apply(m, rows, turns, tiles):
            here, up, down = rows
            for q in range(3):
                h = [powers[m, q, 0, l, here, :] for l in range(3)]
                u = [powers[m, q, 1, l, here, :] for l in range(3)]
                slope_h, slope_u = dx(h), dx(u)
                turn = rotation[turns, :]
                for l in range(tiles):
                    ha, hb = powers[m, q, 0, l, up, :], powers[m, q, 0, l, down, :]
                    va, vb = powers[m, q, 2, l, up, :], powers[m, q, 2, l, down, :]
                    v = powers[m, q, 2, l, here, :]
                    powers[m + 1, q, 0, l, here, :] = slope_u[l] + (va - vb)
                    powers[m + 1, q, 1, l, here, :] = slope_h[l] - turn * v
                    powers[m + 1, q, 2, l, here, :] = (ha - hb) + turn * u[l]

        def next_power(m, carry):
            apply(m, (tall, above, below), turns, 3)
            return carry

        for m in range(CHEB - 1):
            next_power(m, 0)
        apply(CHEB - 1, at(HALO + block_start, block_count), pl.ds(pl.multiple_of(HALO + block_start, 8), block_count), 2)

    most, rest = REST * (1 - late), MOST * late
    await_bytes(y_bytes, HALO_Y)
    await_side(1 - late)
    spread_edges(HALO * (1 - late), TALL - HALO)
    all_powers(HALO * (1 - late), TALL - HALO, most, MOST)

    for i in range(5, 8):
        @pl.when((1 - earlier[i]) * at_end == 1)
        def _(i=i):
            send_to_later(i)

    @pl.when(last)
    def _():
        @pl.when(gy == 0)
        def _():
            opening[1].start()

    block = pl.ds(BASE, ROWS)

    class Part:
        def __init__(self, start, count):
            self.rows = pl.ds(pl.multiple_of(start, 8), count)
            self.source = pl.ds(pl.multiple_of(BASE + start, 8), count)
            self.size = pl.ds(0, count)

    large, small, whole = Part(most, MOST), Part(rest, REST), Part(0, ROWS)

    def mix(part, f, wanted):
        def body(l, carry):
            totals = [None] * len(wanted)
            for q in range(3):
                for m in range(CHEB + 1):
                    value = powers[m, q, f, l, part.source, :]
                    for i, (delta, p, _, _) in enumerate(wanted):
                        term = weight(delta, p, q, m) * value
                        totals[i] = term if totals[i] is None else totals[i] + term
            for (delta, p, ref, index), total in zip(wanted, totals, strict=True):
                if delta:
                    total = total * jnp.where(tm + delta >= n_tm, circulant, 1.0).astype(F32)
                ref[(*index, l, part.rows, slice(None))] = total
            return carry
        for l in range(2):
            body(l, 0)

    def both_steps(delta, ref, *index):
        return [(delta, p, ref, (*index, p)) for p in range(2)]

    def odd_delta(seat, place):
        return (2 * place + 1 - 2 * seat) % 8

    def for_partner(part, f, places):
        for seat in range(2):
            @pl.when(core == seat)
            def _(seat=seat):
                mix(part, f, [w for place in places for w in both_steps(odd_delta(seat, place), cross, place, f)])

    def send_across(part, f, place, i):
        remote(cross.at[place, f, :, :, part.rows, :], crossed.at[place, f, :, :, part.rows, :], sem.at[CROSS_S], sem.at[i],
               (partner, gx, gy)).start()

    up, down = (chip_up, gx, gy), (chip_down, gx, gy)

    def send_ring(i, side, src, dst):
        remote(src, dst, sem.at[RING_S], sem.at[i], down if side else up).start()

    def add_into(part, f, place, i, other):
        own[i, f, :, :, part.rows, :] = own[i, f, :, :, part.rows, :] + crossed[other, f, :, :, part.rows, :]

    def send_far(part, f, i):
        for side in range(2):
            send_ring(i, side, own.at[0, f, side, :, part.rows, :], relay.at[side, f, :, part.rows, :])

    def send_near(part, f, i):
        for side in range(2):
            send_ring(i, side, own.at[1 + side, f, 1 - side, :, part.rows, :], near_a.at[side, f, :, part.rows, :])

    def send_relayed(part, f, i):
        for side in range(2):
            send_ring(i, side, own.at[1 + side, f, side, :, part.rows, :], near_b.at[side, f, :, part.rows, :])

    def add_relayed(part, f):
        for side in range(2):
            own[1 + side, f, side, :, part.rows, :] = (
                own[1 + side, f, side, :, part.rows, :] + relay[side, f, :, part.rows, :])

    def each_field(body):
        def step(f, carry):
            body(f)
            return carry
        lax.fori_loop(0, 3, step, 0)

    def far_odd(f):
        for_partner(large, f, (2,))
        send_across(large, f, 2, CROSS_FAR + f)

    def far_out(f):
        for_partner(large, f, (1, 3))
        send_across(large, f, 1, CROSS_NEAR + f)
        send_across(large, f, 3, CROSS_NEAR + f)
        await_bytes(crossed.at[2, f, :, :, large.size, :], CROSS_FAR + f)
        add_into(large, f, 2, 0, 2)
        send_far(large, f, RING_FAR + f)

    def near_out(f):
        mix(large, f, both_steps(2, own, 1, f) + both_steps(6, own, 2, f))
        await_bytes(crossed.at[pl.ds(0, 2), f, :, :, large.size, :], CROSS_NEAR + f)
        add_into(large, f, 1, 1, 1)
        add_into(large, f, 3, 2, 3)
        send_near(large, f, RING_END)

    def relay_out(f):
        await_bytes(relay.at[:, f, :, large.size, :], RING_FAR + f)
        add_relayed(large, f)
        send_relayed(large, f, RING_END)

    def here_odd(f):
        for_partner(whole, f, (0,))
        send_across(whole, f, 0, CROSS_OWN)

    each_field(far_odd)
    each_field(lambda f: mix(large, f, both_steps(4, own, 0, f)))
    each_field(far_out)

    await_side(late)
    spread_edges((HALO + ROWS) * late, HALO)
    all_powers(ROWS * late, 2 * HALO, rest, REST)

    fields = slice(None)
    each_field(lambda f: for_partner(small, f, (2,)))
    send_across(small, fields, 2, CROSS_FAR + 3)
    each_field(near_out)
    each_field(lambda f: mix(small, f, both_steps(4, own, 0, f)))
    await_bytes(crossed.at[2, :, :, :, small.size, :], CROSS_FAR + 3)
    add_into(small, fields, 2, 0, 2)
    send_far(small, fields, RING_FAR + 3)
    each_field(lambda f: for_partner(small, f, (1, 3)))
    send_across(small, fields, 1, CROSS_NEAR + 3)
    send_across(small, fields, 3, CROSS_NEAR + 3)
    each_field(lambda f: mix(small, f, both_steps(2, own, 1, f) + both_steps(6, own, 2, f)))
    each_field(relay_out)
    await_bytes(crossed.at[pl.ds(0, 2), :, :, :, small.size, :], CROSS_NEAR + 3)
    add_into(small, fields, 1, 1, 1)
    add_into(small, fields, 3, 2, 3)
    send_near(small, fields, RING_END)
    each_field(here_odd)
    await_bytes(relay.at[:, :, :, small.size, :], RING_FAR + 3)
    add_relayed(small, fields)
    send_relayed(small, fields, RING_END)
    each_field(lambda f: mix(whole, f, both_steps(0, own, 3, f)))

    await_bytes(prev, PASS_R)
    await_bytes(crossed.at[0], CROSS_OWN)
    for f in range(3):
        for l in range(2):
            before_first = jnp.where(tm == 0, state[2, f, l, block, :], prev[f, l])
            res_buf[0, f, l] = powers[0, 0, f, l, block, :] - before_first
            res_buf[1, f, l] = powers[0, 1, f, l, block, :]
            for p in range(2):
                out_buf[p, f, l] = state[p, f, l, block, :] - (own[3, f, p, l] + crossed[0, f, p, l])

    await_bytes(halo_bytes, HALO_S)

    @pl.when(last)
    def _():
        await_bytes(opening_bytes, OPEN_S)

    await_bytes(prev, PASS_S)
    await_bytes(cross, CROSS_S)

    await_bytes(own.at[pl.ds(0, 2)], RING_END)
    for p in range(2):
        out_buf[p] = out_buf[p] - (near_b[p] + near_a[1 - p])
    await_bytes(own.at[pl.ds(0, 3)], RING_S)


def put_out(upd_in, res_in, upd_out, res_out, sem):
    copies = []
    for l in range(2):
        columns = pl.ds(128 * l, 128)
        copies.append(pltpu.make_async_copy(upd_in.at[:, :, l], upd_out.at[:, :, :, columns], sem.at[l]))
        copies.append(pltpu.make_async_copy(res_in.at[:, :, l], res_out.at[:, :, :, columns], sem.at[2 + l]))
    for copy in copies:
        copy.start()
    for copy in copies:
        copy.wait()


def shards(trajectory, initial):
    whole = jax.ShapeDtypeStruct(trajectory.shape, F32)
    anywhere = pl.BlockSpec(memory_space=pl.ANY)
    slow = pl.BlockSpec(memory_space=pltpu.HBM)
    fast = pl.BlockSpec(memory_space=pltpu.VMEM)
    dma = pltpu.SemaphoreType.DMA
    tiles = pltpu.VMEM((2, 3, 2, ROWS, 128), F32)
    updated, residual = pl.pallas_call(
        kernel,
        out_shape=(tiles, tiles),
        in_specs=[slow, slow],
        out_specs=(fast, fast),
        scratch_shapes=[
            pltpu.VMEM((3, 3, 3, DEEP, 128), F32),
            pltpu.VMEM((CHEB + 1, 3, 3, 3, DEEP, 128), F32),
            pltpu.VMEM((TALL, 128), F32),
            pltpu.VMEM((3, 2, ROWS, 128), F32),
            pltpu.VMEM((ROWS, 128), F32),
            pltpu.VMEM((ROWS, 128), F32),
            pltpu.VMEM((TALL, 128), F32),
            pltpu.VMEM((TALL, 128), F32),
            pltpu.VMEM((2, 3, 3, 2, HALO, 128), F32),
            pltpu.VMEM((4, 3, 2, 2, ROWS, 128), F32),
            pltpu.VMEM((4, 3, 2, 2, ROWS, 128), F32),
            pltpu.VMEM((4, 3, 2, 2, ROWS, 128), F32),
            pltpu.VMEM((2, 3, 2, ROWS, 128), F32),
            pltpu.VMEM((2, 3, 2, ROWS, 128), F32),
            pltpu.VMEM((2, 3, 2, ROWS, 128), F32),
            pltpu.SemaphoreType.REGULAR((9,)),
            dma((N_SEM,)),
        ],
        compiler_params=pltpu.CompilerParams(collective_id=0, has_side_effects=True),
        name="paradiag",
    )(trajectory, initial)
    return pl.pallas_call(
        put_out,
        out_shape=(whole, whole),
        in_specs=[anywhere, anywhere],
        out_specs=(anywhere, anywhere),
        scratch_shapes=[dma((4,))],
        compiler_params=pltpu.CompilerParams(vmem_limit_bytes=4 << 20),
        name="put_out",
    )(updated, residual)


def solution(mesh):
    in_specs = (P("tm", None, "gy", "gx"), P(None, "gy", "gx"))
    out_specs = (P("tm", None, "gy", "gx"), P("tm", None, "gy", "gx"))
    return jax.shard_map(shards, mesh=mesh, in_specs=in_specs, out_specs=out_specs, check_vma=False)
```

```python
import math

import jax
import jax.numpy as jnp
import numpy as np
from jax import lax
from jax.experimental import pallas as pl
from jax.experimental.pallas import tpu as pltpu
from jax.sharding import PartitionSpec as P

MESH = pl.DeviceIdType.MESH
F32 = jnp.float32

CHEB = 6
STEPS = 16
courant = 1.5
coriolis_mean = 0.3
coriolis_slope = 0.4
circulant = 0.1
spectrum_edge = 5.0

HALO = 8
ROWS = 32
TALL = ROWS + 2 * HALO
EDGE = 8
BASE = EDGE + HALO
DEEP = TALL + 2 * EDGE
WRAPS = 1.0 / circulant
OPPOSITE = (1, 0, 5, 6, 7, 2, 3, 4, 8, 8, 8, 8, 8)
MOST, REST = 24, 8
(LOAD, HALO_S, HALO_Y, HALO_SIDE, OPEN_S, OPEN_SIDE, PASS_S, PASS_R, CROSS_S, RING_S, CROSS_FAR, CROSS_NEAR, CROSS_OWN, RING_FAR,
 RING_END, N_SEM) = (0, 1, 2, 3, 5, 6, 8, 9, 10, 11, 12, 16, 20, 21, 25, 26)


def power_table():
    beta = circulant ** (1.0 / STEPS)
    solved = np.zeros((STEPS, CHEB + 1), complex)
    for k in range(STEPS):
        theta = 2.0 * np.pi * k / STEPS
        shift = 1.0 - beta * np.cos(theta) + 1j * beta * np.sin(theta)
        edge = 1j * spectrum_edge
        sigma = shift / edge
        rho_old = 1.0 / sigma
        one = np.zeros(CHEB + 2, complex)
        one[0] = 1.0
        update = one / shift
        total = update.copy()
        for _ in range(CHEB):
            misfit = one - (shift * total + np.roll(total, 1))
            rho_new = 1.0 / (2.0 * sigma - rho_old)
            update = rho_new * rho_old * update + 2.0 * rho_new / edge * misfit
            total = total + update
            rho_old = rho_new
        solved[k] = total[: CHEB + 1]
    turns = np.exp(2j * np.pi / STEPS * np.outer(np.arange(STEPS), np.arange(STEPS)))
    table = (turns @ solved).real / STEPS
    return table * courant ** np.arange(CHEB + 1)


TABLE = power_table()


def weight(delta, p, q, m):
    difference = 2 * delta + p - q
    return float(circulant ** (-difference / STEPS) * TABLE[difference % STEPS, m])


def kernel(
    traj, init, out_buf, res_buf,
    state, powers, rotation, prev, strip_l, strip_r, edge_l, edge_r,
    side_in, cross, crossed, own, relay, relay_odd, near_a, near_b,
    ready, sem,
):
    tm, gx, gy = lax.axis_index("tm"), lax.axis_index("gx"), lax.axis_index("gy")
    n_tm, n_gx, n_gy = lax.axis_size("tm"), lax.axis_size("gx"), lax.axis_size("gy")
    core = lax.rem(tm, 2)
    east, west = lax.rem(gx + 1, n_gx), lax.rem(gx + n_gx - 1, n_gx)
    north, south = lax.rem(gy + 1, n_gy), lax.rem(gy + n_gy - 1, n_gy)
    after = lax.rem(tm + 1, n_tm)
    chip_up, chip_down = lax.rem(tm + 2, n_tm), lax.rem(tm + n_tm - 2, n_tm)
    partner = tm + 1 - 2 * core
    last = tm == n_tm - 1

    loads = []
    for lane in range(2):
        columns = pl.ds(128 * lane, 128)
        loads.append(pltpu.make_async_copy(
            traj.at[:, :, :, columns], state.at[pl.ds(0, 2), :, lane, pl.ds(BASE, ROWS), :], sem.at[LOAD]))
        loads.append(pltpu.make_async_copy(
            init.at[:, :, columns], state.at[2, :, lane, pl.ds(BASE, ROWS), :], sem.at[LOAD]))
    for load in loads:
        load.start()
    loaded = state.at[:, :, pl.ds(0, 2), pl.ds(BASE, ROWS), :]

    up_other, down_other = chip_up + 1 - 2 * core, chip_down + 1 - 2 * core
    peers = [(tm, east, gy), (tm, west, gy), (tm, gx, north), (tm, east, north), (tm, west, north),
             (tm, gx, south), (tm, west, south), (tm, east, south),
             (partner, gx, gy), (chip_up, gx, gy), (chip_down, gx, gy), (up_other, gx, gy), (down_other, gx, gy)]
    chip = lax.div(tm, 2)
    next_chip, prior_chip = lax.rem(chip + 1, n_tm // 2), lax.rem(chip + n_tm // 2 - 1, n_tm // 2)

    def key_t(its_chip, its_core):
        return (its_chip + 1 - its_core) * 256 + (2 * its_chip + its_core) * 32

    def key_z(y):
        return jnp.minimum(2 * y + 2 * jnp.minimum(y, 1), 11) * 256 + y

    mine_t, mine_x, mine_z = key_t(chip, core), gx * 264, key_z(gy)
    east_x, west_x, north_z, south_z = east * 264, west * 264, key_z(north), key_z(south)
    mine = mine_t + mine_x + mine_z
    keys = [mine_t + east_x + mine_z, mine_t + west_x + mine_z, mine_t + mine_x + north_z, mine_t + east_x + north_z,
            mine_t + west_x + north_z, mine_t + mine_x + south_z, mine_t + west_x + south_z, mine_t + east_x + south_z,
            key_t(chip, 1 - core) + mine_x + mine_z, key_t(next_chip, core) + mine_x + mine_z,
            key_t(prior_chip, core) + mine_x + mine_z,
            key_t(next_chip, 1 - core) + mine_x + mine_z, key_t(prior_chip, 1 - core) + mine_x + mine_z]
    earlier = [(key < mine).astype(jnp.int32) for key in keys]

    barrier = pltpu.get_barrier_semaphore()
    for peer, sooner in zip(peers, earlier, strict=True):
        @pl.when(sooner == 0)
        def _(peer=peer):
            pl.semaphore_signal(barrier, inc=1, device_id=peer, device_id_type=MESH)

    sooner_count = sum(earlier)

    @pl.when(sooner_count > 0)
    def _():
        pl.semaphore_wait(barrier, sooner_count)

    for i, (peer, sooner) in enumerate(zip(peers, earlier, strict=True)):
        @pl.when(sooner == 1)
        def _(i=i, peer=peer):
            pl.semaphore_signal(ready.at[OPPOSITE[i]], inc=1, device_id=peer, device_id_type=MESH)

    pltpu.make_async_copy(loaded, loaded, sem.at[LOAD]).wait()

    lane_id = lax.broadcasted_iota(jnp.int32, (TALL, 128), 1)
    def remote(src, dst, send, recv, peer):
        return pltpu.make_async_remote_copy(
            src_ref=src, dst_ref=dst, send_sem=send, recv_sem=recv, device_id=peer, device_id_type=MESH)

    top, bottom, low, high = pl.ds(0, HALO), pl.ds(ROWS - HALO, HALO), pl.ds(BASE, HALO), pl.ds(EDGE + ROWS, HALO)
    first, final = pl.ds(0, HALO), pl.ds(HALO + ROWS, HALO)
    both, cols = pl.ds(0, 2), pl.ds(0, 2)
    middle = pl.ds(HALO, ROWS)
    sides = [
        (strip_r, edge_l.at[middle]),
        (strip_l, edge_r.at[middle]),
        (state.at[both, :, cols, high, :], side_in.at[0, both]),
        (strip_r.at[bottom], edge_l.at[first]),
        (strip_l.at[bottom], edge_r.at[first]),
        (state.at[both, :, cols, low, :], side_in.at[1, both]),
        (strip_l.at[top], edge_r.at[final]),
        (strip_r.at[top], edge_l.at[final]),
    ]
    seats = (HALO_Y, HALO_Y, HALO_SIDE, HALO_SIDE, HALO_SIDE, HALO_SIDE + 1, HALO_SIDE + 1, HALO_SIDE + 1)
    halo = [remote(src, dst, sem.at[HALO_S], sem.at[seats[i]], peers[i]) for i, (src, dst) in enumerate(sides)]
    opening = [
        remote(state.at[2, :, cols, high, :], side_in.at[0, 2], sem.at[OPEN_S], sem.at[OPEN_SIDE],
               (tm, gx, north)),
        remote(state.at[2, :, cols, low, :], side_in.at[1, 2], sem.at[OPEN_S], sem.at[OPEN_SIDE + 1],
               (tm, gx, south)),
    ]
    passed = remote(state.at[1, :, cols, pl.ds(BASE, ROWS), :], prev, sem.at[PASS_S], sem.at[PASS_R], (after, gx, gy))
    def send_to_earlier(i):
        @pl.when(earlier[i] == 1)
        def _():
            halo[i].start()

    for i in (2, 5):
        send_to_earlier(i)

    packed_l = jnp.zeros((ROWS, 128), F32)
    packed_r = jnp.zeros((ROWS, 128), F32)
    for s in range(3):
        for f in range(3):
            spot = 8 * (3 * s + f)
            here = (lane_id[:ROWS] >= spot) & (lane_id[:ROWS] < spot + 8)
            left = state[s, f, 0, pl.ds(BASE, ROWS), :]
            right = state[s, f, 1, pl.ds(BASE, ROWS), :]
            packed_l = jnp.where(here, pltpu.roll(left, spot, 1) if spot else left, packed_l)
            packed_r = jnp.where(here, pltpu.roll(right, spot + 8, 1), packed_r)
    strip_l[...] = packed_l
    strip_r[...] = packed_r

    for i in (0, 1, 3, 4, 6, 7):
        send_to_earlier(i)

    def send_to_later(i):
        pl.semaphore_wait(ready.at[i], 1)
        halo[i].start()

    at_end = 1 - jnp.minimum(gy, 1)
    for i in range(8):
        @pl.when(earlier[i] + (at_end if i >= 5 else 0) == 0)
        def _(i=i):
            send_to_later(i)

    @pl.when(last)
    def _():
        opening[0].start()

        @pl.when(gy > 0)
        def _():
            opening[1].start()

    later_count = 5 - sum(earlier[8:])

    @pl.when(later_count > 0)
    def _():
        pl.semaphore_wait(ready.at[8], later_count)

    passed.start()

    def await_bytes(ref, i):
        pltpu.make_async_copy(ref, ref, sem.at[i]).wait()

    halo_bytes, y_bytes = state.at[:, :, 0, pl.ds(0, ROWS), :], relay.at[0, 0]
    side_bytes = powers.at[:, 0, 0, 0, pl.ds(0, 2 * HALO), :]
    opening_bytes, opening_side = state.at[2, :, cols, pl.ds(0, 2 * HALO), :], state.at[2, :, cols, pl.ds(0, HALO), :]

    late = jnp.minimum(gy, 1)

    def await_side(side):
        await_bytes(side_bytes, HALO_SIDE + side)

        @pl.when(last)
        def _():
            await_bytes(opening_side, OPEN_SIDE + side)

        state[:, :, cols, pl.ds(pl.multiple_of(EDGE + (HALO + ROWS) * side, 8), HALO), :] = side_in[side]

    row = (gy * ROWS - HALO + n_gy * ROWS + lax.broadcasted_iota(jnp.int32, (TALL, 128), 0)) % (n_gy * ROWS)
    latitude = coriolis_mean + coriolis_slope * ((row.astype(F32) + 0.5) / (n_gy * ROWS) - 0.5)
    rotation[...] = latitude * (1.0 / courant)

    def spread_edges(start, count):
        here = pl.ds(pl.multiple_of(start, 8), count)
        there = pl.ds(pl.multiple_of(EDGE + start, 8), count)
        for s in range(3):
            for f in range(3):
                spot = 8 * (3 * s + f)
                packed = edge_r[here, :]
                right = pltpu.roll(packed, (128 - spot) % 128, 1) if spot else packed
                left = pltpu.roll(edge_l[here, :], 120 - spot, 1)
                state[s, f, 2, there, :] = jnp.where(lane_id[:count] < 64, right, left)

    def dx(tiles):
        ahead = [pltpu.roll(t, 127, 1) for t in tiles]
        behind = [pltpu.roll(t, 1, 1) for t in tiles]
        lane = lane_id[: tiles[0].shape[0]]
        return [jnp.where(lane == 127, ahead[(l + 1) % 3], ahead[l]) - jnp.where(lane == 0, behind[(l + 2) % 3], behind[l])
                for l in range(3)]

    def all_powers(start, count, block_start, block_count):
        def at(first_row, rows):
            begin = pl.multiple_of(EDGE + first_row, 8)
            return pl.ds(begin, rows), pl.ds(begin + 1, rows), pl.ds(begin - 1, rows)

        tall, above, below = at(start, count)
        turns = pl.ds(pl.multiple_of(start, 8), count)

        def start_fields(s, carry):
            h = [state[s, 0, l, tall, :] for l in range(3)]
            u = [state[s, 1, l, tall, :] for l in range(3)]
            v = [state[s, 2, l, tall, :] for l in range(3)]
            turn = rotation[turns, :]
            flux = dx([u[l] + h[l] * u[l] for l in range(3)])
            slope_h, slope_u, slope_v = dx(h), dx(u), dx(v)
            for l in range(3):
                (ha, hb), (ua, ub), (va, vb) = [(state[s, f, l, above, :], state[s, f, l, below, :]) for f in range(3)]
                powers[0, s, 0, l, tall, :] = h[l] + courant * (flux[l] + ((va + ha * va) - (vb + hb * vb)))
                powers[0, s, 1, l, tall, :] = u[l] + courant * (
                    slope_h[l] - turn * v[l] + (u[l] * slope_u[l] + v[l] * (ua - ub)))
                powers[0, s, 2, l, tall, :] = v[l] + courant * (
                    (ha - hb) + turn * u[l] + (u[l] * slope_v[l] + v[l] * (va - vb)))
            return carry

        for s in range(2):
            start_fields(s, 0)

        slot = jnp.where(last, 2, 1)
        factor = jnp.where(last, -WRAPS, -1.0).astype(F32)
        for f in range(3):
            for l in range(3):
                powers[0, 2, f, l, tall, :] = factor * state[slot, f, l, tall, :]
                powers[0, 1, f, l, tall, :] = powers[0, 1, f, l, tall, :] - state[0, f, l, tall, :]

        def apply(m, rows, turns, tiles):
            here, up, down = rows
            for q in range(3):
                h = [powers[m, q, 0, l, here, :] for l in range(3)]
                u = [powers[m, q, 1, l, here, :] for l in range(3)]
                slope_h, slope_u = dx(h), dx(u)
                turn = rotation[turns, :]
                for l in range(tiles):
                    ha, hb = powers[m, q, 0, l, up, :], powers[m, q, 0, l, down, :]
                    va, vb = powers[m, q, 2, l, up, :], powers[m, q, 2, l, down, :]
                    v = powers[m, q, 2, l, here, :]
                    powers[m + 1, q, 0, l, here, :] = slope_u[l] + (va - vb)
                    powers[m + 1, q, 1, l, here, :] = slope_h[l] - turn * v
                    powers[m + 1, q, 2, l, here, :] = (ha - hb) + turn * u[l]

        def next_power(m, carry):
            apply(m, (tall, above, below), turns, 3)
            return carry

        for m in range(CHEB - 1):
            next_power(m, 0)
        apply(CHEB - 1, at(HALO + block_start, block_count), pl.ds(pl.multiple_of(HALO + block_start, 8), block_count), 2)

    most, rest = REST * (1 - late), MOST * late
    await_bytes(y_bytes, HALO_Y)
    await_side(1 - late)
    spread_edges(HALO * (1 - late), TALL - HALO)
    all_powers(HALO * (1 - late), TALL - HALO, most, MOST)

    for i in range(5, 8):
        @pl.when((1 - earlier[i]) * at_end == 1)
        def _(i=i):
            send_to_later(i)

    @pl.when(last)
    def _():
        @pl.when(gy == 0)
        def _():
            opening[1].start()

    block = pl.ds(BASE, ROWS)

    class Part:
        def __init__(self, start, count):
            self.rows = pl.ds(pl.multiple_of(start, 8), count)
            self.source = pl.ds(pl.multiple_of(BASE + start, 8), count)
            self.size = pl.ds(0, count)

    large, small, whole = Part(most, MOST), Part(rest, REST), Part(0, ROWS)

    def mix(part, f, wanted):
        def body(l, carry):
            totals = [None] * len(wanted)
            for q in range(3):
                for m in range(CHEB + 1):
                    value = powers[m, q, f, l, part.source, :]
                    for i, (delta, p, _, _) in enumerate(wanted):
                        term = weight(delta, p, q, m) * value
                        totals[i] = term if totals[i] is None else totals[i] + term
            for (delta, p, ref, index), total in zip(wanted, totals, strict=True):
                if delta:
                    total = total * jnp.where(tm + delta >= n_tm, circulant, 1.0).astype(F32)
                ref[(*index, l, part.rows, slice(None))] = total
            return carry
        for l in range(2):
            body(l, 0)

    def both_steps(delta, ref, *index):
        return [(delta, p, ref, (*index, p)) for p in range(2)]

    def odd_delta(seat, place):
        return (2 * place + 1 - 2 * seat) % 8

    def for_partner(part, f, places):
        for seat in range(2):
            @pl.when(core == seat)
            def _(seat=seat):
                mix(part, f, [w for place in places for w in both_steps(odd_delta(seat, place), cross, place, f)])

    def send_across(part, f, place, i):
        remote(cross.at[place, f, :, :, part.rows, :], crossed.at[place, f, :, :, part.rows, :], sem.at[CROSS_S], sem.at[i],
               (partner, gx, gy)).start()

    up, down = (chip_up, gx, gy), (chip_down, gx, gy)

    def send_ring(i, side, src, dst):
        remote(src, dst, sem.at[RING_S], sem.at[i], down if side else up).start()

    def add_into(part, f, place, i, other):
        own[i, f, :, :, part.rows, :] = own[i, f, :, :, part.rows, :] + crossed[other, f, :, :, part.rows, :]

    def send_far(part, f, i):
        for side in range(2):
            send_ring(i, side, own.at[0, f, side, :, part.rows, :], relay.at[side, f, :, part.rows, :])

    def send_near(part, f, i):
        for side in range(2):
            send_ring(i, side, own.at[1 + side, f, 1 - side, :, part.rows, :], near_a.at[side, f, :, part.rows, :])

    def send_relayed(part, f, i):
        for side in range(2):
            send_ring(i, side, own.at[1 + side, f, side, :, part.rows, :], near_b.at[side, f, :, part.rows, :])

    def add_relayed(part, f):
        for side in range(2):
            own[1 + side, f, side, :, part.rows, :] = (
                own[1 + side, f, side, :, part.rows, :] + relay[side, f, :, part.rows, :])

    def each_field(body, start=0):
        def step(f, carry):
            body(f)
            return carry
        lax.fori_loop(start, 3, step, 0)

    def far_odd(f):
        for_partner(large, f, (2,))
        send_across(large, f, 2, CROSS_FAR + f)

    def near_odd(f):
        for_partner(large, f, (1, 3))
        send_across(large, f, 1, CROSS_NEAR + f)
        send_across(large, f, 3, CROSS_NEAR + f)

    def far_out(f):
        near_odd(f)
        await_bytes(crossed.at[2, f, :, :, large.size, :], CROSS_FAR + f)
        add_into(large, f, 2, 0, 2)
        send_far(large, f, RING_FAR + f)

    def near_out(f):
        mix(large, f, both_steps(2, own, 1, f) + both_steps(6, own, 2, f))
        await_bytes(crossed.at[pl.ds(0, 2), f, :, :, large.size, :], CROSS_NEAR + f)
        add_into(large, f, 1, 1, 1)
        add_into(large, f, 3, 2, 3)
        send_near(large, f, RING_END)

    def relay_first():
        await_bytes(own.at[pl.ds(0, 2), 0, :, :, large.size, :], RING_FAR)
        for side in range(2):
            relay[side, 0, :, large.rows, :] = relay[side, 0, :, large.rows, :] + relay_odd[side, :, large.rows, :]
        add_relayed(large, 0)
        send_relayed(large, 0, RING_END)

    def relay_out(f):
        await_bytes(relay.at[:, f, :, large.size, :], RING_FAR + f)
        add_relayed(large, f)
        send_relayed(large, f, RING_END)

    def here_odd(f):
        for_partner(whole, f, (0,))
        send_across(whole, f, 0, CROSS_OWN)

    for_partner(large, 0, (2,))
    for side, other in enumerate((up_other, down_other)):
        remote(cross.at[2, 0, side, :, large.rows, :], relay_odd.at[side, :, large.rows, :], sem.at[CROSS_S],
               sem.at[RING_FAR], (other, gx, gy)).start()
    mix(large, 0, both_steps(4, own, 0, 0))
    send_far(large, 0, RING_FAR)
    each_field(far_odd, 1)
    each_field(lambda f: mix(large, f, both_steps(4, own, 0, f)), 1)
    near_odd(0)
    each_field(far_out, 1)

    await_side(late)
    spread_edges((HALO + ROWS) * late, HALO)
    all_powers(ROWS * late, 2 * HALO, rest, REST)

    fields = slice(None)
    each_field(lambda f: for_partner(small, f, (2,)))
    send_across(small, fields, 2, CROSS_FAR + 3)
    each_field(near_out)
    each_field(lambda f: mix(small, f, both_steps(4, own, 0, f)))
    await_bytes(crossed.at[2, :, :, :, small.size, :], CROSS_FAR + 3)
    add_into(small, fields, 2, 0, 2)
    send_far(small, fields, RING_FAR + 3)
    each_field(lambda f: for_partner(small, f, (1, 3)))
    send_across(small, fields, 1, CROSS_NEAR + 3)
    send_across(small, fields, 3, CROSS_NEAR + 3)
    each_field(lambda f: mix(small, f, both_steps(2, own, 1, f) + both_steps(6, own, 2, f)))
    relay_first()
    each_field(relay_out, 1)
    await_bytes(crossed.at[pl.ds(0, 2), :, :, :, small.size, :], CROSS_NEAR + 3)
    add_into(small, fields, 1, 1, 1)
    add_into(small, fields, 3, 2, 3)
    send_near(small, fields, RING_END)
    each_field(here_odd)
    await_bytes(relay.at[:, :, :, small.size, :], RING_FAR + 3)
    add_relayed(small, fields)
    send_relayed(small, fields, RING_END)
    each_field(lambda f: mix(whole, f, both_steps(0, own, 3, f)))

    await_bytes(prev, PASS_R)
    await_bytes(crossed.at[0], CROSS_OWN)
    for f in range(3):
        for l in range(2):
            before_first = jnp.where(tm == 0, state[2, f, l, block, :], prev[f, l])
            res_buf[0, f, l] = powers[0, 0, f, l, block, :] - before_first
            res_buf[1, f, l] = powers[0, 1, f, l, block, :]
            for p in range(2):
                out_buf[p, f, l] = state[p, f, l, block, :] - (own[3, f, p, l] + crossed[0, f, p, l])

    await_bytes(halo_bytes, HALO_S)

    @pl.when(last)
    def _():
        await_bytes(opening_bytes, OPEN_S)

    await_bytes(prev, PASS_S)
    await_bytes(cross, CROSS_S)

    await_bytes(own.at[pl.ds(0, 2)], RING_END)
    for p in range(2):
        out_buf[p] = out_buf[p] - (near_b[p] + near_a[1 - p])
    await_bytes(own.at[pl.ds(0, 3)], RING_S)


def put_out(upd_in, res_in, upd_out, res_out, sem):
    copies = []
    for l in range(2):
        columns = pl.ds(128 * l, 128)
        copies.append(pltpu.make_async_copy(upd_in.at[:, :, l], upd_out.at[:, :, :, columns], sem.at[l]))
        copies.append(pltpu.make_async_copy(res_in.at[:, :, l], res_out.at[:, :, :, columns], sem.at[2 + l]))
    for copy in copies:
        copy.start()
    for copy in copies:
        copy.wait()


def shards(trajectory, initial):
    whole = jax.ShapeDtypeStruct(trajectory.shape, F32)
    anywhere = pl.BlockSpec(memory_space=pl.ANY)
    slow = pl.BlockSpec(memory_space=pltpu.HBM)
    fast = pl.BlockSpec(memory_space=pltpu.VMEM)
    dma = pltpu.SemaphoreType.DMA
    tiles = pltpu.VMEM((2, 3, 2, ROWS, 128), F32)
    updated, residual = pl.pallas_call(
        kernel,
        out_shape=(tiles, tiles),
        in_specs=[slow, slow],
        out_specs=(fast, fast),
        scratch_shapes=[
            pltpu.VMEM((3, 3, 3, DEEP, 128), F32),
            pltpu.VMEM((CHEB + 1, 3, 3, 3, DEEP, 128), F32),
            pltpu.VMEM((TALL, 128), F32),
            pltpu.VMEM((3, 2, ROWS, 128), F32),
            pltpu.VMEM((ROWS, 128), F32),
            pltpu.VMEM((ROWS, 128), F32),
            pltpu.VMEM((TALL, 128), F32),
            pltpu.VMEM((TALL, 128), F32),
            pltpu.VMEM((2, 3, 3, 2, HALO, 128), F32),
            pltpu.VMEM((4, 3, 2, 2, ROWS, 128), F32),
            pltpu.VMEM((4, 3, 2, 2, ROWS, 128), F32),
            pltpu.VMEM((4, 3, 2, 2, ROWS, 128), F32),
            pltpu.VMEM((2, 3, 2, ROWS, 128), F32),
            pltpu.VMEM((2, 2, ROWS, 128), F32),
            pltpu.VMEM((2, 3, 2, ROWS, 128), F32),
            pltpu.VMEM((2, 3, 2, ROWS, 128), F32),
            pltpu.SemaphoreType.REGULAR((9,)),
            dma((N_SEM,)),
        ],
        compiler_params=pltpu.CompilerParams(collective_id=0, has_side_effects=True),
        name="paradiag",
    )(trajectory, initial)
    return pl.pallas_call(
        put_out,
        out_shape=(whole, whole),
        in_specs=[anywhere, anywhere],
        out_specs=(anywhere, anywhere),
        scratch_shapes=[dma((4,))],
        compiler_params=pltpu.CompilerParams(vmem_limit_bytes=4 << 20),
        name="put_out",
    )(updated, residual)


def solution(mesh):
    in_specs = (P("tm", None, "gy", "gx"), P(None, "gy", "gx"))
    out_specs = (P("tm", None, "gy", "gx"), P("tm", None, "gy", "gx"))
    return jax.shard_map(shards, mesh=mesh, in_specs=in_specs, out_specs=out_specs, check_vma=False)
```
